32 devices in a mesh: groups: 2 (over x), seq: 16 (over z, y, core).
Axes of the slice: x: 2, y: 2, z: 4, core: 2. Of those that a mesh axis runs over, the one named last changes fastest.
Arguments:
- layer_in: bfloat16 [8192, 2560], P(('groups', 'seq')), parts along dimension 0, may hold values from -6 to 6
- ssm_in: bfloat16 [8192, 2560], P(('groups', 'seq')), parts along dimension 0, may hold values from -6 to 6
- weight_bc: bfloat16 [2560, 256], replicated, may hold values from -0.015625 to 0.015625
- weight_dt: bfloat16 [2560, 40], replicated, may hold values from -0.125 to 0.125
- bias_dt: float32 [40], replicated, may hold values from -3 to 0.5
- log_rate: float32 [40], replicated, may hold values from -13.2 to -2.9
- skip_gain: float32 [40], replicated, may hold values from 0.5 to 1.5
- grad_out: bfloat16 [8192, 2560], P(('groups', 'seq')), parts along dimension 0, may hold values from -8 to 8
Outputs:
- grad_ssm_in: bfloat16 [8192, 2560], P(('groups', 'seq')), parts along dimension 0
- grad_layer_in: bfloat16 [8192, 2560], P(('groups', 'seq')), parts along dimension 0
- grad_weight_bc: float32 [5120, 256], P(('groups', 'seq')), parts along dimension 0
- grad_weight_dt: float32 [5120, 40], P(('groups', 'seq')), parts along dimension 0
- grad_bias_dt: float32 [80], P('groups'), parts along dimension 0
- grad_log_rate: float32 [80], P('groups'), parts along dimension 0
- grad_skip_gain: float32 [80], P('groups'), parts along dimension 0
The draws below stay inside these ranges and needn't reach their ends.
There are 2 independent parts, one for each index of `groups`. The reference program is written for one: setup_inputs(seed, part) draws one part's arguments, and reference() takes and returns one part's arrays. A program takes and returns all parts, laid end to end along the dimension named above; an argument that names none is the same for every part. Nothing has to cross between parts.
All inputs are finite; a program needn't handle non-finite values.
Results may differ from the reference program's by a relative error of at most 0.0059.
Values sent between devices are 32-bit elements; how exact they have to be, the bound alone decides.
A program may use at most 128 MiB of HBM per device.

```python
import math
import jax
import jax.numpy as jnp
from jax import lax

D = 2560
HEADS = 40
HEAD_DIM = 64
STATE = 128
BLOCK = 256
LEN = 4096


def draw_log_rate(key, part):
    lowest = math.log(2e-06)
    highest = math.log(0.05)
    return jax.random.uniform(key, (HEADS,), jnp.float32, lowest, highest)


def draw_grad_out(key, part):
    shape = (LEN, HEADS * HEAD_DIM)
    position = jnp.arange(LEN, dtype=jnp.float32)[:, None] / LEN
    base = jnp.clip(jax.random.normal(key, shape, jnp.float32), -5.0, 5.0)
    result = base * (0.5 + position)
    return result.astype(jnp.bfloat16)


def block_levels(stream_key, extent, shards, least, largest):
    level, own = 1.0, jax.random.fold_in(stream_key, 6)
    for dim, blocks in shards:
        heights = jnp.exp(jax.random.uniform(jax.random.fold_in(own, dim), (blocks,), jnp.float32, least / len(shards), largest / len(shards)))
        level = level * jnp.repeat(heights, extent[dim] // blocks).reshape([-1 if axis == dim else 1 for axis in range(len(extent))])
    return level


def noise(stream_key, dims, scale, reach, cuts=(), kind=jnp.bfloat16):
    entries = jax.random.normal(stream_key, dims, jnp.float32) * scale
    if len(cuts) > 0:
        entries = block_levels(stream_key, dims, cuts, -0.22, 0.18) * entries
    return jnp.clip(entries, min=-reach, max=reach).astype(kind)


def setup_inputs(seed: int = 0, part: int = 0) -> dict:
    arg_keys = jax.random.split(jax.random.key(seed), 9)
    part_keys = jax.random.split(jax.random.fold_in(arg_keys[8], part), 9)
    return {
        "layer_in": noise(part_keys[0], (LEN, D), 1.0, 6.0, ((0, 16),)),
        "ssm_in": noise(part_keys[1], (LEN, HEADS * HEAD_DIM), 1.0, 6.0, ((0, 16),)),
        "weight_bc": noise(arg_keys[2], (D, 2 * STATE), (64 * D) ** -0.5, 0.015625),
        "weight_dt": noise(arg_keys[3], (D, HEADS), D ** -0.5, 0.125),
        "bias_dt": jnp.clip(jax.random.uniform(arg_keys[4], (HEADS,), jnp.float32, -3.0, 0.5), -3.0, 0.5),
        "log_rate": draw_log_rate(jax.random.fold_in(arg_keys[8], 71), part),
        "skip_gain": jnp.clip(jax.random.uniform(arg_keys[6], (HEADS,), jnp.float32, 0.5, 1.5), 0.5, 1.5),
        "grad_out": draw_grad_out(jax.random.fold_in(jax.random.fold_in(arg_keys[8], part), 71), part),
    }


HIGHEST = lax.Precision.HIGHEST

def block_pass(state, pieces):
    values, b_rows, c_rows, scores, step_size, log_decay = pieces
    running = jnp.cumsum(log_decay, axis=0)
    count = values.shape[0]
    indices = jnp.arange(count)
    lower_mask = indices[:, None] >= indices[None, :]
    run_heads = running.T
    spread = jnp.where(lower_mask[None, :, :], run_heads[:, :, None] - run_heads[:, None, :], -jnp.inf)
    mixing = jnp.exp(spread) * scores[None, :, :] * step_size.T[:, None, :]
    inner = jnp.einsum('hts,shp->thp', mixing, values, precision=HIGHEST)
    carried = jnp.exp(running)[:, :, None] * jnp.einsum('tn,hpn->thp', c_rows, state, precision=HIGHEST)
    tail_weight = jnp.exp(running[-1][None, :] - running) * step_size
    fresh = jnp.einsum('shp,sn->hpn', tail_weight[:, :, None] * values, b_rows, precision=HIGHEST)
    new_state = jnp.exp(running[-1])[:, None, None] * state + fresh
    return (new_state, inner + carried)

def mixer(values, b_rows, c_rows, scores, step_raw, log_rate, skip_gain):
    step_size = jax.nn.softplus(step_raw)
    log_decay = -jnp.exp(log_rate)[None, :] * step_size
    blocks = values.shape[0] // BLOCK

    def split(array):
        return array.reshape((blocks, BLOCK) + array.shape[1:])
    start = jnp.zeros((values.shape[1], values.shape[2], b_rows.shape[1]), values.dtype)
    final, outputs = lax.scan(jax.checkpoint(block_pass), start, (split(values), split(b_rows), split(c_rows), scores, split(step_size), split(log_decay)))
    return outputs.reshape(values.shape) + skip_gain[None, :, None] * values

def reference(layer_in, ssm_in, weight_bc, weight_dt, bias_dt, log_rate, skip_gain, grad_out):
    length = layer_in.shape[0]
    blocks = length // BLOCK
    proj_bc = jnp.dot(layer_in, weight_bc, preferred_element_type=jnp.float32).astype(jnp.bfloat16)
    proj_kept = lax.optimization_barrier(proj_bc)
    proj_wide = proj_kept.astype(jnp.float32)
    b_rows = proj_wide[:, :STATE]
    c_rows = proj_wide[:, STATE:]
    b_narrow = proj_kept[:, :STATE].reshape(blocks, BLOCK, STATE)
    c_narrow = proj_kept[:, STATE:].reshape(blocks, BLOCK, STATE)
    scores = jnp.einsum('ktn,ksn->kts', c_narrow, b_narrow, preferred_element_type=jnp.float32)
    step_raw = jnp.dot(layer_in, weight_dt, preferred_element_type=jnp.float32) + bias_dt[None, :]
    values = ssm_in.astype(jnp.float32).reshape(length, HEADS, HEAD_DIM)
    primal, pull = jax.vjp(mixer, values, b_rows, c_rows, scores, step_raw, log_rate, skip_gain)
    cotangent = grad_out.astype(jnp.float32).reshape(length, HEADS, HEAD_DIM)
    grad_values, grad_b, grad_c, grad_scores, grad_step, grad_log_rate, grad_skip_gain = pull(cotangent)
    b_blocks = b_rows.reshape(blocks, BLOCK, STATE)
    c_blocks = c_rows.reshape(blocks, BLOCK, STATE)
    grad_b = grad_b + jnp.einsum('kts,ktn->ksn', grad_scores, c_blocks, precision=HIGHEST).reshape(length, STATE)
    grad_c = grad_c + jnp.einsum('kts,ksn->ktn', grad_scores, b_blocks, precision=HIGHEST).reshape(length, STATE)
    grad_bias_dt = lax.optimization_barrier(jnp.sum(grad_step, axis=0))
    grad_bc = jnp.concatenate([grad_b, grad_c], axis=1).astype(jnp.bfloat16)
    grad_dt = grad_step.astype(jnp.bfloat16)
    grad_layer_in = (jnp.dot(grad_bc, weight_bc.T, preferred_element_type=jnp.float32) + jnp.dot(grad_dt, weight_dt.T, preferred_element_type=jnp.float32)).astype(jnp.bfloat16)
    grad_weight_bc = jnp.dot(layer_in.T, grad_bc, preferred_element_type=jnp.float32)
    grad_weight_dt = jnp.dot(layer_in.T, grad_dt, preferred_element_type=jnp.float32)
    grad_ssm_in = grad_values.reshape(length, HEADS * HEAD_DIM).astype(jnp.bfloat16)
    return (grad_ssm_in, grad_layer_in, grad_weight_bc, grad_weight_dt, grad_bias_dt, grad_log_rate, grad_skip_gain)
```

```python
import functools
import jax
import jax.numpy as jnp
from jax import lax
from jax.experimental import pallas as pl
from jax.experimental.pallas import tpu as pltpu
from jax.sharding import PartitionSpec as P

F32 = jnp.float32
BF16 = jnp.bfloat16
TILE = 128
CHUNKS = 5
VMEM_LIMIT = 60 * 1024 * 1024
VMEM = pl.BlockSpec(memory_space=pltpu.VMEM)
ANY = pl.BlockSpec(memory_space=pl.ANY)


def mm(left, right):
    return lax.dot_general(left, right, (((1,), (0,)), ((), ())), preferred_element_type=F32)


def mm_nt(left, right):
    return lax.dot_general(left, right, (((1,), (1,)), ((), ())), preferred_element_type=F32)


def mm_tn(left, right):
    return lax.dot_general(left, right, (((0,), (0,)), ((), ())), preferred_element_type=F32)


def three_way(x):
    high = x.astype(BF16)
    rest = x - high.astype(F32)
    middle = rest.astype(BF16)
    return high, middle, (rest - middle.astype(F32)).astype(BF16)


def one_hot(heads, width, columns, first=0):
    row = lax.broadcasted_iota(jnp.int32, (heads, columns), 0)
    col = lax.broadcasted_iota(jnp.int32, (heads, columns), 1) + first
    inside = (col >= row * width) & (col < (row + 1) * width)
    return jnp.where(inside, 1.0, 0.0).astype(BF16)


def spread(parts, hot):
    return mm(parts[0], hot) + mm(parts[1], hot) + mm(parts[2], hot)


def head_sum(x, hot):
    high = x.astype(BF16)
    low = (x - high.astype(F32)).astype(BF16)
    return mm_nt(high, hot) + mm_nt(low, hot)


def exact_mm(mask, x):
    parts = three_way(x)
    return mm(mask, parts[0]) + mm(mask, parts[1]) + mm(mask, parts[2])


def triangle(size, compare):
    row = lax.broadcasted_iota(jnp.int32, (size, size), 0)
    col = lax.broadcasted_iota(jnp.int32, (size, size), 1)
    return jnp.where(compare(row, col), 1.0, 0.0).astype(BF16)


def inner_pair(pair, heads, u_ref, grad_ref, scores_ref, parts_ref, run_rows_ref,
               gu_ref, rows_ref, gscores_ref, head_size):
    tokens = u_ref.shape[0]
    blocks = tokens // TILE
    per = TILE // head_size
    cols = pl.ds(pl.multiple_of(pair * TILE, TILE), TILE)
    lane = lax.broadcasted_iota(jnp.int32, (TILE, TILE), 1)
    causal = lax.broadcasted_iota(jnp.int32, (TILE, TILE), 0) <= lane
    wide = one_hot(heads, TILE, per * TILE, pair * (per * TILE))
    run_cols = spread([parts_ref[i] for i in range(3)], wide)
    grads = [grad_ref[t * TILE : (t + 1) * TILE, cols] for t in range(blocks)]
    gus = [jnp.zeros((TILE, TILE), F32) for _ in range(blocks)]
    for sub in range(per):
        head = pair * per + sub
        keep = (lane >= sub * head_size) & (lane < (sub + 1) * head_size)
        rows = [jnp.zeros((1, TILE), F32) for _ in range(blocks)]
        for s in range(blocks):
            srange = slice(s * TILE, (s + 1) * TILE)
            run_col = run_cols[srange, sub * TILE : (sub + 1) * TILE]
            u_head = jnp.where(keep, u_ref[srange, cols], jnp.zeros((), BF16))
            gu = jnp.zeros((TILE, TILE), F32)
            for t in range(s, blocks):
                trange = slice(t * TILE, (t + 1) * TILE)
                gap = run_rows_ref[head, :, trange] - run_col
                if s == t:
                    gap = jnp.where(causal, gap, -jnp.inf)
                factor = jnp.exp(gap)
                mixing = (factor * scores_ref[srange, trange]).astype(BF16)
                weight = mm_nt(u_head, grads[t])
                gscores_ref[srange, trange] += factor * weight
                rows[t] += jnp.sum(mixing.astype(F32) * weight, axis=0, keepdims=True)
                gu += mm(mixing, grads[t])
            gus[s] = jnp.where(keep, gu, gus[s])
        for t in range(blocks):
            rows_ref[head, :, t * TILE : (t + 1) * TILE] = rows[t]
    for s in range(blocks):
        gu_ref[s * TILE : (s + 1) * TILE, cols] = gus[s]


def packing(depth, devices, heads):
    share = depth // devices
    lanes = TILE // heads
    group = -(-share // (8 * lanes)) * 8
    return share, lanes, group


def reduce_plan(depth, devices, heads):
    share, lanes, group = packing(depth, devices, heads)
    levels = devices.bit_length() - 1
    y_first = list(range(levels))
    z_first = [0] + list(range(2, levels)) + [1]
    pieces = 2 if share % 32 == 0 else 1
    plan = []
    for plane, order in ((1, z_first), (0, y_first)):
        for piece in range(pieces):
            size = share // pieces
            plan.append((plane, piece * size, size, order))
    plan.append((2, 0, group + 8, y_first))
    return plan


def scratch_list(tokens, depth, width, heads, state_dim, devices):
    levels = devices.bit_length() - 1
    half, quarter = state_dim // 2, state_dim // 4
    plan = reduce_plan(depth, devices, heads)
    names = {}

    def add(name, shape, dtype=F32):
        names[name] = pltpu.VMEM(shape, dtype)

    add("layer", (tokens, depth), BF16)
    add("values", (tokens, width), BF16)
    add("grad", (tokens, width), BF16)
    add("wbc", (depth, 2 * state_dim), BF16)
    add("wdt", (heads, depth), BF16)
    add("layer_t", (depth, tokens), BF16)
    add("proj", (tokens, 2 * state_dim), BF16)
    add("proj_t", (2 * state_dim, tokens), BF16)
    add("hot", (TILE, width), BF16)
    add("parts", (3, tokens, heads), BF16)
    for name in ("raw", "step", "run"):
        add(name, (tokens, heads))
    add("run_rows", (heads, 1, tokens))
    add("rows", (heads, 1, tokens))
    add("scores", (tokens, tokens))
    add("gscores", (tokens, tokens))
    for name in ("step_w", "lead_w", "tail_w", "gu"):
        add(name, (tokens, width))
    for name in ("u", "tsv", "lg"):
        add(name, (tokens, width), BF16)
    for name in ("reads", "cols", "backs", "gsteps"):
        add(name, (tokens, heads))
    add("cross", (8, heads))
    add("skips", (8, heads))
    add("gc", (tokens, state_dim))
    add("gb", (tokens, state_dim))
    add("gproj", (tokens, 2 * state_dim + heads), BF16)
    add("gvalues", (tokens, width), BF16)
    add("glayer", (tokens, depth), BF16)
    for kind in ("s", "g"):
        add("st_" + kind, (state_dim, width))
        add("get0_" + kind, (half, width))
        add("agg1_" + kind, (half, width))
        add("get1_" + kind, (quarter, width))
        add("agg2_" + kind, (quarter, width))
        add("zin_" + kind, (quarter, width))
        add("zout_" + kind, (quarter, width))
        add("send1_" + kind, (quarter, width))
        add("chip_" + kind, (half, width))
        add("send0_" + kind, (half, width))
        add("end_" + kind, (state_dim, width))
    add("tots", (2, 8, TILE))
    add("tot_gets", (2, 8, TILE))
    add("decays", (5, 8, width))
    for q, (plane, first, size, order) in enumerate(plan):
        add(f"sum{q}", (devices * size, TILE))
        for i in range(levels):
            add(f"rget{q}_{i}", ((devices >> (i + 1)) * size, TILE))
    add_sem = lambda name, shape: names.__setitem__(name, pltpu.SemaphoreType.DMA(shape))
    add_sem("load", (5,))
    add_sem("store", (2,))
    add_sem("comm", (2, 5, 2, CHUNKS))
    add_sem("tot_sems", (2, 2))
    add_sem("rsem", (2, levels, len(plan)))
    return names


class Box:
    pass


def mega_kernel(devices, names, layer_hbm, values_hbm, wbc_hbm, wdt_hbm, bias_ref, rate_ref,
                gain_ref, grad_hbm, gvalues_hbm, glayer_hbm, gbc_ref, last_ref, *refs):
    r = Box()
    for name, ref in zip(names, refs):
        setattr(r, name, ref)
    tokens, depth = r.layer.shape
    width = r.values.shape[1]
    heads = bias_ref.shape[1]
    head_size = width // heads
    state_dim = r.st_s.shape[0]
    half, quarter = state_dim // 2, state_dim // 4
    levels = devices.bit_length() - 1
    zrows = devices // 4
    span = width // CHUNKS
    me = lax.axis_index("seq")
    bits = [lax.rem(me // (1 << k), 2) for k in range(levels)]
    partners = [me + (1 - 2 * bits[k]) * (1 << k) for k in range(levels)]
    row = me // 4
    up_row = lax.rem(me + 4, devices)
    down_row = lax.rem(me + devices - 4, devices)
    mesh_id = pl.DeviceIdType.MESH

    loads = [
        pltpu.make_async_copy(source, target, r.load.at[i])
        for i, (source, target) in enumerate((
            (layer_hbm, r.layer), (wbc_hbm, r.wbc), (wdt_hbm, r.wdt),
            (values_hbm, r.values), (grad_hbm, r.grad),
        ))
    ]
    for load in loads:
        load.start()

    barrier = pltpu.get_barrier_semaphore()
    for k in range(levels):
        pl.semaphore_signal(barrier, inc=1, device_id={"seq": partners[k]}, device_id_type=mesh_id)
    if zrows > 1:
        @pl.when(row < zrows - 1)
        def _():
            pl.semaphore_signal(barrier, inc=1, device_id={"seq": up_row}, device_id_type=mesh_id)

        @pl.when(row > 0)
        def _():
            pl.semaphore_signal(barrier, inc=1, device_id={"seq": down_row}, device_id_type=mesh_id)

    r.hot[...] = one_hot(TILE, head_size, width)
    loads[0].wait()
    loads[1].wait()
    layer = r.layer[...]
    proj = mm(layer, r.wbc[...]).astype(BF16)
    r.proj[...] = proj
    r.proj_t[...] = proj.T
    loads[2].wait()
    raw = mm_nt(layer, r.wdt[...]) + bias_ref[...]
    r.raw[...] = raw
    step = jnp.maximum(raw, 0.0) + jnp.log1p(jnp.exp(-jnp.abs(raw)))
    r.step[...] = step
    decay = -jnp.exp(rate_ref[...]) * step
    run = exact_mm(triangle(tokens, lambda a, b: a >= b), decay)
    r.run[...] = run
    total = run[tokens - 1 :, :]
    r.tots[0] = jnp.zeros((8, TILE), F32)
    r.tots[0, :, :heads] = jnp.broadcast_to(total, (8, heads))
    if zrows > 1:
        count = levels + jnp.where(row < zrows - 1, 1, 0) + jnp.where(row > 0, 1, 0)
    else:
        count = levels
    pl.semaphore_wait(barrier, count)

    def remote(source, target, send, receive, device):
        return pltpu.make_async_remote_copy(
            src_ref=source, dst_ref=target, send_sem=send, recv_sem=receive,
            device_id={"seq": device}, device_id_type=mesh_id,
        )

    def tot_copy(k):
        return remote(r.tots.at[k], r.tot_gets.at[k], r.tot_sems.at[0, k], r.tot_sems.at[1, k],
                      partners[k])

    tot_copy(0).start()

    kinds = ("s", "g")

    def cols_of(k):
        return slice(k * span, (k + 1) * span)

    def at(name, kind):
        return getattr(r, name + "_" + kind)

    def rows_at(which, size):
        return pl.ds(pl.multiple_of(which * size, 8), size)

    def copy(stage, kind, k):
        cols = cols_of(k)
        if stage == 0:
            source = at("st", kind).at[rows_at(1 - bits[0], half), cols]
            target, device = at("get0", kind).at[:, cols], partners[0]
        elif stage == 1:
            source = at("agg1", kind).at[rows_at(1 - bits[1], quarter), cols]
            target, device = at("get1", kind).at[:, cols], partners[1]
        elif stage == 2:
            source, target = at("zout", kind).at[:, cols], at("zin", kind).at[:, cols]
            device = up_row if kind == "s" else down_row
        elif stage == 3:
            source = at("send1", kind).at[:, cols]
            target, device = at("chip", kind).at[rows_at(bits[1], quarter), cols], partners[1]
        else:
            source = at("send0", kind).at[:, cols]
            target, device = at("end", kind).at[rows_at(bits[0], half), cols], partners[0]
        i = kinds.index(kind)
        return remote(source, target, r.comm.at[0, stage, i, k], r.comm.at[1, stage, i, k], device)

    def tot_done(k):
        tot_copy(k).wait_recv()
        mine, other = r.tots[k], r.tot_gets[k]
        both = jnp.concatenate([mine, other], axis=0)
        stacked = jnp.concatenate(list(three_way(both)), axis=0)
        wide = mm(stacked, r.hot[...])
        wide = jnp.exp(wide[0:16] + wide[16:32] + wide[32:48])
        r.decays[2 * k] = wide[0:8]
        r.decays[2 * k + 1] = wide[8:16]
        if k == 0:
            r.tots[1] = mine + other
            tot_copy(1).start()
        else:
            r.decays[4] = wide[0:8] * wide[8:16]

    first0, first1 = bits[0] == 0, bits[1] == 0

    def make_states(kind, k):
        if k == 0:
            loads[3 if kind == "s" else 4].wait()
        cols = cols_of(k)
        hot = r.hot[:heads, cols]
        if kind == "s":
            step_w = spread(three_way(r.step[...]), hot)
            r.step_w[:, cols] = step_w
            run = r.run[...]
            tail_w = spread(three_way(jnp.exp(run[tokens - 1 :, :] - run)), hot)
            r.tail_w[:, cols] = tail_w
            u = step_w * r.values[:, cols].astype(F32)
            r.u[:, cols] = u.astype(BF16)
            tsv = (tail_w * u).astype(BF16)
            r.tsv[:, cols] = tsv
            r.st_s[:, cols] = mm(r.proj_t[:state_dim], tsv)
        else:
            lead_w = spread(three_way(jnp.exp(r.run[...])), hot)
            r.lead_w[:, cols] = lead_w
            lg = (lead_w * r.grad[:, cols].astype(F32)).astype(BF16)
            r.lg[:, cols] = lg
            r.st_g[:, cols] = mm(r.proj_t[state_dim:], lg)
        copy(0, kind, k).start()

    def merge(kind, first, mine, got, e_mine, e_other):
        if kind == "s":
            return jnp.where(first, e_other * mine + got, mine + e_mine * got)
        return jnp.where(first, mine + e_mine * got, e_other * mine + got)

    def split(kind, first, parent, mine, got, e_mine, e_other):
        far, near = e_other * parent + got, e_mine * parent + mine
        if kind == "s":
            return jnp.where(first, parent, far), jnp.where(first, near, parent)
        return jnp.where(first, far, parent), jnp.where(first, parent, near)

    def pair_up(kind, k):
        if kind == "s" and k == 0:
            tot_done(0)
        copy(0, kind, k).wait_recv()
        cols = cols_of(k)
        mine = at("st", kind)[rows_at(bits[0], half), cols]
        got = at("get0", kind)[:, cols]
        at("agg1", kind)[:, cols] = merge(
            kind, first0, mine, got, r.decays[0, 0:1, cols], r.decays[1, 0:1, cols])
        copy(1, kind, k).start()

    def row_up(kind, k):
        if kind == "s" and k == 0:
            tot_done(1)
        copy(1, kind, k).wait_recv()
        cols = cols_of(k)
        mine = at("agg1", kind)[rows_at(bits[1], quarter), cols]
        got = at("get1", kind)[:, cols]
        at("agg2", kind)[:, cols] = merge(
            kind, first1, mine, got, r.decays[2, 0:1, cols], r.decays[3, 0:1, cols])

    def chain(kind, k, place):
        cols = cols_of(k)
        if place > 0:
            copy(2, kind, k).wait_recv()
            parent = at("zin", kind)[:, cols]
        else:
            parent = jnp.zeros((quarter, span), F32)
        if place < zrows - 1:
            passed = at("agg2", kind)[:, cols]
            if place > 0:
                passed = r.decays[4, 0:1, cols] * parent + passed
            at("zout", kind)[:, cols] = passed
            copy(2, kind, k).start()
        mine = at("agg1", kind)[rows_at(bits[1], quarter), cols]
        got = at("get1", kind)[:, cols]
        kept, sent = split(kind, first1, parent, mine, got,
                           r.decays[2, 0:1, cols], r.decays[3, 0:1, cols])
        at("send1", kind)[:, cols] = sent
        copy(3, kind, k).start()
        at("chip", kind)[rows_at(bits[1], quarter), cols] = kept

    def chain_slot(kind, k, place):
        where = place if kind == "s" else zrows - 1 - place
        if zrows == 1:
            chain(kind, k, place)
        else:
            pl.when(row == where)(lambda: chain(kind, k, place))

    def chip_down(kind, k):
        copy(3, kind, k).wait_recv()
        cols = cols_of(k)
        parent = at("chip", kind)[:, cols]
        mine = at("st", kind)[rows_at(bits[0], half), cols]
        got = at("get0", kind)[:, cols]
        kept, sent = split(kind, first0, parent, mine, got,
                           r.decays[0, 0:1, cols], r.decays[1, 0:1, cols])
        at("send0", kind)[:, cols] = sent
        copy(4, kind, k).start()
        at("end", kind)[rows_at(bits[0], half), cols] = kept

    def gather(name, k, x):
        ref = getattr(r, name)
        ref[...] = x if k == 0 else ref[...] + x

    def forward_tail(k):
        copy(4, "s", k).wait_recv()
        cols = cols_of(k)
        hot = r.hot[:heads, cols]
        inc = r.end_s[:, cols].astype(BF16)
        lead_grad = r.lead_w[:, cols] * r.grad[:, cols].astype(F32)
        gather("reads", k, head_sum(lead_grad * mm(r.proj[:, state_dim:], inc), hot))
        gather("gc", k, mm_nt(r.lg[:, cols], inc))

    def inner_tail(k):
        cols = cols_of(k)
        hot = r.hot[:heads, cols]
        gather("cols", k, head_sum(r.u[:, cols].astype(F32) * r.gu[:, cols], hot))
        products = r.values[:, cols].astype(F32) * r.grad[:, cols].astype(F32)
        products = jnp.sum(products, axis=0, keepdims=True)
        gather("skips", k, head_sum(jnp.broadcast_to(products, (8, span)), hot))

    def backward_tail(k):
        copy(4, "g", k).wait_recv()
        cols = cols_of(k)
        hot = r.hot[:heads, cols]
        outgoing = r.end_g[:, cols]
        out = outgoing.astype(BF16)
        values = r.values[:, cols].astype(F32)
        gather("gb", k, mm_nt(r.tsv[:, cols], out))
        back = r.tail_w[:, cols] * mm(r.proj[:, :state_dim], out)
        gather("backs", k, head_sum(values * back, hot))
        gu = r.gu[:, cols] + back
        gather("gsteps", k, head_sum(values * gu, hot))
        cross = jnp.sum(r.end_s[:, cols] * outgoing, axis=0, keepdims=True)
        gather("cross", k, head_sum(jnp.broadcast_to(cross, (8, span)), hot))
        gain = spread(three_way(jnp.broadcast_to(gain_ref[...], (8, heads))), hot)[0:1]
        r.gvalues[:, cols] = (
            r.step_w[:, cols] * gu + gain * r.grad[:, cols].astype(F32)
        ).astype(BF16)

    plan = reduce_plan(depth, devices, heads)
    share, lanes, group = packing(depth, devices, heads)

    def places(order):
        return [
            sum(((shard >> order[i]) & 1) * (devices >> (i + 1)) for i in range(levels))
            for shard in range(devices)
        ]

    def offset(order, count):
        result = 0
        for i in range(count):
            result = result + bits[order[i]] * (devices >> (i + 1))
        return result

    def part(q, i, which):
        size, order = plan[q][2], plan[q][3]
        start = (offset(order, i) + which * (devices >> (i + 1))) * size
        return pl.ds(pl.multiple_of(start, 8), (devices >> (i + 1)) * size)

    def reduce_copy(q, i):
        k = plan[q][3][i]
        return remote(
            getattr(r, f"sum{q}").at[part(q, i, 1 - bits[k])], getattr(r, f"rget{q}_{i}"),
            r.rsem.at[0, i, q], r.rsem.at[1, i, q], partners[k],
        )

    def reduce_step(q, i):
        k = plan[q][3][i]
        reduce_copy(q, i).wait_recv()
        sums = getattr(r, f"sum{q}")
        mine = part(q, i, bits[k])
        sums[mine] = sums[mine] + getattr(r, f"rget{q}_{i}")[...]
        if i + 1 < levels:
            reduce_copy(q, i + 1).start()

    def plane_start(plane, product):
        for q, (owner, first, size, order) in enumerate(plan):
            if owner != plane:
                continue
            sums = getattr(r, f"sum{q}")
            where = places(order)
            for shard in range(devices):
                start = shard * share + first
                sums[where[shard] * size : (where[shard] + 1) * size] = product[start : start + size]
            reduce_copy(q, 0).start()

    def finish_c():
        grad_c = r.gc[...] + mm_tn(r.gscores[...].astype(BF16), r.proj[:, :state_dim])
        grad_c = grad_c.astype(BF16)
        r.gproj[:, state_dim : 2 * state_dim] = grad_c
        plane_start(1, mm(r.layer_t[...], grad_c))

    def finish_b():
        grad_b = r.gb[...] + mm(r.gscores[...].astype(BF16), r.proj[:, state_dim:])
        grad_b = grad_b.astype(BF16)
        r.gproj[:, :state_dim] = grad_b
        plane_start(0, mm(r.layer_t[...], grad_b))

    def finish_dt():
        raw, step, run = r.raw[...], r.step[...], r.run[...]
        rate = jnp.exp(rate_ref[...])
        total = run[tokens - 1 :, :]
        upper = triangle(tokens, lambda a, b: a <= b)
        lower = triangle(tokens, lambda a, b: a > b)
        inner = r.rows[:, 0, :].T + r.reads[...] - r.cols[...]
        grad_decay = (
            exact_mm(upper, inner) + exact_mm(lower, step * r.backs[...])
            + jnp.exp(total) * r.cross[0:1]
        )
        sigmoid = 1.0 / (1.0 + jnp.exp(-raw))
        grad_raw = (r.gsteps[...] - rate * grad_decay) * sigmoid
        narrow = grad_raw.astype(BF16)
        r.gproj[:, 2 * state_dim :] = narrow
        shift_row = lax.broadcasted_iota(jnp.int32, (heads, lanes * TILE), 0)
        shift_col = lax.broadcasted_iota(jnp.int32, (heads, lanes * TILE), 1)
        shift = jnp.zeros(shift_row.shape, F32)
        for j in range(lanes):
            shift = jnp.where(shift_col == shift_row + j * (TILE + heads), 1.0, shift)
        moved = mm(narrow, shift.astype(BF16)).astype(BF16)
        product = mm(r.layer_t[...], moved)
        q = len(plan) - 1
        unit = group + 8
        sums = getattr(r, f"sum{q}")
        where = places(plan[q][3])
        small = jnp.concatenate([
            jnp.sum(grad_raw, axis=0, keepdims=True),
            -rate * jnp.sum(grad_decay * step, axis=0, keepdims=True),
            r.skips[0:1],
            jnp.zeros((5, heads), F32),
        ], axis=0)
        small = jnp.concatenate([small, jnp.zeros((8, TILE - heads), F32)], axis=1)
        for shard in range(devices):
            start = where[shard] * unit
            packed = jnp.zeros((group, TILE), F32)
            for j in range(lanes):
                count = min(share - j * group, group)
                if count <= 0:
                    continue
                first = shard * share + j * group
                piece = product[first : first + count, j * TILE : (j + 1) * TILE]
                if count < group:
                    piece = jnp.concatenate(
                        [piece, jnp.zeros((group - count, TILE), F32)], axis=0)
                packed = packed + piece
            sums[start : start + group] = packed
            sums[start + group : start + unit] = small
        reduce_copy(q, 0).start()

    def layer_tail():
        r.glayer[...] = (
            mm_nt(r.gproj[:, : 2 * state_dim], r.wbc[...])
            + mm(r.gproj[:, 2 * state_dim :], r.wdt[...])
        ).astype(BF16)
        stores[1].start()

    stores = [
        pltpu.make_async_copy(r.gvalues, gvalues_hbm, r.store.at[0]),
        pltpu.make_async_copy(r.glayer, glayer_hbm, r.store.at[1]),
    ]

    def prepare():
        run = r.run[...]
        run_rows = run.T
        for head in range(heads):
            r.run_rows[head] = run_rows[head : head + 1]
        for i, piece in enumerate(three_way(run)):
            r.parts[i] = piece
        r.scores[...] = mm_nt(r.proj[:, :state_dim], r.proj[:, state_dim:])
        r.gscores[...] = jnp.zeros_like(r.gscores)

    def turn():
        r.layer_t[...] = r.layer[...].T

    def body(pair, _):
        inner_pair(pair, heads, r.u, r.grad, r.scores, r.parts, r.run_rows,
                   r.gu, r.rows, r.gscores, head_size)
        return 0

    events = []

    def event(time, work, *args):
        events.append((time, len(events), functools.partial(work, *args)))

    n = CHUNKS
    make, wire, flight, near, hop = 0.5, 1.5, 2.3, 1.4, 3.7
    base = make + near
    for k in range(n):
        event(make * k, make_states, "s", k)
        event(make * (k + 1) + near, pair_up, "s", k)
        event(make * (n + k), make_states, "g", k)
        event(make * (n + k + 1) + near, pair_up, "g", k)
        for i, kind in enumerate(kinds):
            arrive = base + wire * (i * n + k + 1) + flight
            event(arrive, row_up, kind, k)
            for place in range(zrows):
                event(arrive + hop * min(place, 3) + 0.01, chain_slot, kind, k, place)
            back = base + wire * ((2 + i) * n + k + 1) + flight
            event(back + 0.1, chip_down, kind, k)
            event(back + near, forward_tail if kind == "s" else backward_tail, k)
    event(make * 2 * n + 0.05, prepare)
    event(make * 2 * n + 8.0, turn)
    c_time = base + wire * 3 * n + flight + near + 0.2
    inner_time = base + wire * 2 * n + flight
    for k in range(n):
        event(inner_time + 0.02 * k, inner_tail, k)
    event(c_time, finish_c)
    b_time = base + wire * 4 * n + flight + near + 0.2
    event(b_time, finish_b)
    event(b_time + 0.1, stores[0].start)
    event(b_time + 0.2, finish_dt)
    event(b_time + 0.3, layer_tail)
    for q, (plane, first, size, order) in enumerate(plan):
        time = (c_time if plane == 1 else b_time + 1.0) + 0.2
        if plane == 2:
            time = time + 0.4
        piece = 1 if first > 0 else 0
        pace = 3.6 * size / 80
        for i in range(levels):
            if i == 0:
                time = time + 1.4 + 0.5 * piece
            else:
                time = time + pace * (1 + piece * (i == 1)) + 2.3
                pace = pace / 2
            event(time, reduce_step, q, i)
    events.sort(key=lambda item: item[:2])

    pairs = width // TILE
    pair_time = 0.42
    done, clock, begun = 0, 0.0, False
    for time, index, work in events:
        if begun and done < pairs:
            take = min(pairs - done, int((time - clock) / pair_time))
            if time >= inner_time:
                take = pairs - done
            if take >= 2 or (take > 0 and done + take == pairs):
                lax.fori_loop(done, done + take, body, 0)
                done += take
                clock = clock + take * pair_time
        work()
        clock = max(clock, time)
        if work.func is prepare:
            begun = True
            clock = time + 0.3

    for q, (plane, first, size, order) in enumerate(plan):
        unit = size
        start = pl.multiple_of(offset(order, levels) * unit, 8)
        result = getattr(r, f"sum{q}")[pl.ds(start, unit)]
        if plane < 2:
            gbc_ref[first : first + size, plane * TILE : (plane + 1) * TILE] = result
        else:
            last_ref[...] = result
    for store in stores:
        store.wait()
    for k in range(2):
        tot_copy(k).wait_send()
    for kind in kinds:
        for k in range(n):
            for stage in (0, 1, 3, 4):
                copy(stage, kind, k).wait_send()
        if zrows > 1:
            sends = row < zrows - 1 if kind == "s" else row > 0

            @pl.when(sends)
            def _(kind=kind):
                for k in range(n):
                    copy(2, kind, k).wait_send()
    for q in range(len(plan)):
        for i in range(levels):
            reduce_copy(q, i).wait_send()


def finish_kernel(heads, group, lanes, gvalues_in, glayer_in, gbc_in, last_in,
                  gvalues_ref, glayer_ref, gbc_ref, gdt_ref, gbias_ref, grate_ref, gskip_ref):
    gvalues_ref[...] = gvalues_in[...]
    glayer_ref[...] = glayer_in[...]
    gbc_ref[...] = gbc_in[...]
    last = last_in[...]
    share = gdt_ref.shape[0]
    for j in range(lanes):
        count = min(share - j * group, group)
        if count > 0:
            gdt_ref[j * group : j * group + count] = last[:count, j * heads : (j + 1) * heads]
    gbias_ref[...] = last[group : group + 1, :heads]
    grate_ref[...] = last[group + 1 : group + 2, :heads]
    gskip_ref[...] = last[group + 2 : group + 3, :heads]


def local(layer_in, ssm_in, weight_bc, weight_dt, bias_dt, log_rate, skip_gain, grad_out):
    tokens, depth = layer_in.shape
    heads = log_rate.shape[0]
    width = ssm_in.shape[1]
    state_dim = weight_bc.shape[1] // 2
    devices = lax.axis_size("seq")
    share, lanes, group = packing(depth, devices, heads)
    scratch = scratch_list(tokens, depth, width, heads, state_dim, devices)
    shape = jax.ShapeDtypeStruct
    gvalues, glayer, gbc, last = pl.pallas_call(
        functools.partial(mega_kernel, devices, list(scratch)),
        out_shape=[
            shape((tokens, width), BF16),
            shape((tokens, depth), BF16),
            shape((share, 2 * state_dim), F32),
            shape((group + 8, TILE), F32),
        ],
        in_specs=[ANY] * 4 + [VMEM] * 3 + [ANY],
        out_specs=[ANY, ANY, VMEM, VMEM],
        scratch_shapes=list(scratch.values()),
        compiler_params=pltpu.CompilerParams(
            collective_id=0, has_side_effects=True, vmem_limit_bytes=VMEM_LIMIT
        ),
        name="mixer",
    )(layer_in, ssm_in, weight_bc, weight_dt.T, bias_dt[None, :], log_rate[None, :],
      skip_gain[None, :], grad_out)
    outs = pl.pallas_call(
        functools.partial(finish_kernel, heads, group, lanes),
        out_shape=[
            shape((tokens, width), BF16),
            shape((tokens, depth), BF16),
            shape((share, 2 * state_dim), F32),
            shape((share, heads), F32),
            shape((1, heads), F32),
            shape((1, heads), F32),
            shape((1, heads), F32),
        ],
        in_specs=[VMEM] * 4,
        out_specs=[VMEM] * 7,
        compiler_params=pltpu.CompilerParams(vmem_limit_bytes=VMEM_LIMIT),
        name="finish",
    )(gvalues, glayer, gbc, last)
    return tuple(outs[:4]) + tuple(out[0] for out in outs[4:])


def solution(mesh):
    rows = P(("groups", "seq"), None)
    in_specs = (rows, rows, P(), P(), P(), P(), P(), rows)
    out_specs = (rows, rows, rows, rows, P("groups"), P("groups"), P("groups"))
    return jax.shard_map(local, mesh=mesh, in_specs=in_specs, out_specs=out_specs, check_vma=False)
```

```python
import functools
import jax
import jax.numpy as jnp
from jax import lax
from jax.experimental import pallas as pl
from jax.experimental.pallas import tpu as pltpu
from jax.sharding import PartitionSpec as P

F32 = jnp.float32
BF16 = jnp.bfloat16
TILE = 128
CHUNKS = 10
BLOCK = 2
REDUCE_C, REDUCE_B, REDUCE_DT = "zzyy", "yyyy", "z"
VMEM_LIMIT = 52 * 1024 * 1024
VMEM = pl.BlockSpec(memory_space=pltpu.VMEM)
ANY = pl.BlockSpec(memory_space=pl.ANY)


def mm(left, right):
    return lax.dot_general(left, right, (((1,), (0,)), ((), ())), preferred_element_type=F32)


def mm_nt(left, right):
    return lax.dot_general(left, right, (((1,), (1,)), ((), ())), preferred_element_type=F32)


def mm_tn(left, right):
    return lax.dot_general(left, right, (((0,), (0,)), ((), ())), preferred_element_type=F32)


def three_way(x):
    high = x.astype(BF16)
    rest = x - high.astype(F32)
    middle = rest.astype(BF16)
    return high, middle, (rest - middle.astype(F32)).astype(BF16)


def one_hot(heads, width, columns, first=0):
    row = lax.broadcasted_iota(jnp.int32, (heads, columns), 0)
    col = lax.broadcasted_iota(jnp.int32, (heads, columns), 1) + first
    inside = (col >= row * width) & (col < (row + 1) * width)
    return jnp.where(inside, 1.0, 0.0).astype(BF16)


def one_hot_stacked(heads, width, columns, first=0):
    row = lax.rem(lax.broadcasted_iota(jnp.int32, (TILE, columns), 0), heads)
    real = lax.broadcasted_iota(jnp.int32, (TILE, columns), 0) < 3 * heads
    col = lax.broadcasted_iota(jnp.int32, (TILE, columns), 1) + first
    inside = (col >= row * width) & (col < (row + 1) * width) & real
    return jnp.where(inside, 1.0, 0.0).astype(BF16)


def stacked(x):
    rows, heads = x.shape
    zero = jnp.zeros((rows, TILE - heads), F32)
    result = None
    for i, piece in enumerate(three_way(x)):
        piece = jnp.concatenate([piece.astype(F32), zero], axis=1)
        piece = piece if i == 0 else pltpu.roll(piece, i * heads, 1)
        result = piece if i == 0 else result + piece
    return result.astype(BF16)


def head_sum(x, hot):
    high = x.astype(BF16)
    low = (x - high.astype(F32)).astype(BF16)
    return mm_nt(high, hot) + mm_nt(low, hot)


def exact_mm(mask, x):
    parts = three_way(x)
    return mm(mask, parts[0]) + mm(mask, parts[1]) + mm(mask, parts[2])


def triangle(size, compare):
    row = lax.broadcasted_iota(jnp.int32, (size, size), 0)
    col = lax.broadcasted_iota(jnp.int32, (size, size), 1)
    return jnp.where(compare(row, col), 1.0, 0.0).astype(BF16)


def inner_pair(pair, heads, u_ref, grad_ref, scores_ref, parts_ref, run_rows_ref,
               gu_ref, rows_ref, gscores_ref, head_size):
    tokens = u_ref.shape[0]
    blocks = tokens // TILE
    per = TILE // head_size
    cols = pl.ds(pl.multiple_of(pair * TILE, TILE), TILE)
    lane = lax.broadcasted_iota(jnp.int32, (TILE, TILE), 1)
    causal = lax.broadcasted_iota(jnp.int32, (TILE, TILE), 0) <= lane
    wide = one_hot_stacked(heads, TILE, per * TILE, pair * (per * TILE))
    run_cols = mm(parts_ref[...], wide)
    grads = [grad_ref[t * TILE : (t + 1) * TILE, cols] for t in range(blocks)]
    gus = [jnp.zeros((TILE, TILE), F32) for _ in range(blocks)]
    for sub in range(per):
        head = pair * per + sub
        keep = (lane >= sub * head_size) & (lane < (sub + 1) * head_size)
        rows = [jnp.zeros((1, TILE), F32) for _ in range(blocks)]
        for s in range(blocks):
            srange = slice(s * TILE, (s + 1) * TILE)
            run_col = run_cols[srange, sub * TILE : (sub + 1) * TILE]
            u_head = jnp.where(keep, u_ref[srange, cols], jnp.zeros((), BF16))
            gu = jnp.zeros((TILE, TILE), F32)
            for t in range(s, blocks):
                trange = slice(t * TILE, (t + 1) * TILE)
                gap = run_rows_ref[head, :, trange] - run_col
                if s == t:
                    gap = jnp.where(causal, gap, -jnp.inf)
                factor = jnp.exp(gap)
                mixing = (factor * scores_ref[srange, trange]).astype(BF16)
                weight = mm_nt(u_head, grads[t])
                gscores_ref[srange, trange] += factor * weight
                rows[t] += jnp.sum(mixing.astype(F32) * weight, axis=0, keepdims=True)
                gu += mm(mixing, grads[t])
            gus[s] = jnp.where(keep, gu, gus[s])
        for t in range(blocks):
            rows_ref[head, :, t * TILE : (t + 1) * TILE] = rows[t]
    for s in range(blocks):
        gu_ref[s * TILE : (s + 1) * TILE, cols] = gus[s]


def packing(depth, devices, heads):
    share = depth // devices
    lanes = TILE // heads
    group = -(-share // (8 * lanes)) * 8
    return share, lanes, group


def pieces_of(share):
    units = share // 16
    if share % 16 or units < 4:
        return [share]
    return [16 * ((units + 3 - i) // 4) for i in range(4)]


def reduce_plan(depth, devices, heads):
    share, lanes, group = packing(depth, devices, heads)
    levels = devices.bit_length() - 1
    y_first = list(range(levels))
    z_first = [0] + list(range(2, levels)) + [1]
    plan, first = [], 0
    cuts = pieces_of(share)
    for plane, names in ((1, REDUCE_C), (0, REDUCE_B)):
        first = 0
        for piece, size in enumerate(cuts):
            plan.append((plane, first, size, y_first if names[piece] == "y" else z_first))
            first += size
    plan.append((2, 0, group + 8, y_first if REDUCE_DT == "y" else z_first))
    return plan


def scratch_list(tokens, depth, width, heads, state_dim, devices):
    levels = devices.bit_length() - 1
    half, quarter = state_dim // 2, state_dim // 4
    plan = reduce_plan(depth, devices, heads)
    names = {}

    def add(name, shape, dtype=F32):
        names[name] = pltpu.VMEM(shape, dtype)

    add("layer", (tokens, depth), BF16)
    add("values", (tokens, width), BF16)
    add("grad", (tokens, width), BF16)
    add("wbc", (depth, 2 * state_dim), BF16)
    add("wdt", (heads, depth), BF16)
    add("layer_t", (depth, tokens), BF16)
    add("proj", (tokens, 2 * state_dim), BF16)
    add("proj_t", (2 * state_dim, tokens), BF16)
    add("hot", (TILE, width), BF16)
    for name in ("parts", "step3", "tail3", "lead3"):
        add(name, (tokens, TILE), BF16)
    add("hot3", (TILE, width), BF16)
    for name in ("bias", "rate", "gain"):
        add(name, (1, heads))
    add("pre", (tokens, heads))
    add("sigmoid", (tokens, heads))
    for name in ("raw", "step", "run"):
        add(name, (tokens, heads))
    add("run_rows", (heads, 1, tokens))
    add("rows", (heads, 1, tokens))
    add("scores", (tokens, tokens))
    add("gscores", (tokens, tokens))
    for name in ("step_w", "lead_w", "tail_w", "gu"):
        add(name, (tokens, width))
    for name in ("u", "tsv", "lg"):
        add(name, (tokens, width), BF16)
    for name in ("reads", "cols", "backs", "gsteps"):
        add(name, (tokens, heads))
    add("cross", (8, heads))
    add("skips", (8, heads))
    add("small", (8, TILE))
    add("gc", (tokens, state_dim))
    add("gb", (tokens, state_dim))
    add("gproj", (tokens, 2 * state_dim + heads), BF16)
    for kind in ("s", "g"):
        add("st_" + kind, (state_dim, width))
        add("get0_" + kind, (half, width))
        add("agg1_" + kind, (half, width))
        add("get1_" + kind, (quarter, width))
        add("agg2_" + kind, (quarter, width))
        add("zin_" + kind, (quarter, width))
        add("zout_" + kind, (quarter, width))
        add("send1_" + kind, (quarter, width))
        add("chip_" + kind, (half, width))
        add("send0_" + kind, (half, width))
        add("end_" + kind, (state_dim, width))
    add("tots", (2, 8, TILE))
    add("tot_gets", (2, 8, TILE))
    add("decays", (5, 8, width))
    for q, (plane, first, size, order) in enumerate(plan):
        add(f"sum{q}", (devices * size, TILE))
        for i in range(levels):
            add(f"rget{q}_{i}", ((devices >> (i + 1)) * size, TILE))
    add_sem = lambda name, shape: names.__setitem__(name, pltpu.SemaphoreType.DMA(shape))
    add_sem("load", (8,))
    add_sem("comm", (2, 5, 2, CHUNKS))
    add_sem("tot_sems", (2, 2))
    add_sem("rsem", (2, levels, len(plan)))
    return names


class Box:
    pass


def mega_kernel(devices, names, layer_hbm, values_hbm, wbc_hbm, wdt_hbm, bias_hbm, rate_hbm,
                gain_hbm, grad_hbm, gvalues_ref, glayer_ref, gbc_ref, last_ref, *refs):
    r = Box()
    for name, ref in zip(names, refs):
        setattr(r, name, ref)
    tokens, depth = r.layer.shape
    width = r.values.shape[1]
    heads = r.bias.shape[1]
    head_size = width // heads
    state_dim = r.st_s.shape[0]
    half, quarter = state_dim // 2, state_dim // 4
    levels = devices.bit_length() - 1
    zrows = devices // 4
    span = width // CHUNKS
    me = lax.axis_index("seq")
    bits = [lax.rem(me // (1 << k), 2) for k in range(levels)]
    partners = [me + (1 - 2 * bits[k]) * (1 << k) for k in range(levels)]
    row = me // 4
    up_row = lax.rem(me + 4, devices)
    down_row = lax.rem(me + devices - 4, devices)
    mesh_id = pl.DeviceIdType.MESH

    loads = [
        pltpu.make_async_copy(source, target, r.load.at[i])
        for i, (source, target) in enumerate((
            (layer_hbm, r.layer), (wbc_hbm, r.wbc), (wdt_hbm, r.wdt),
            (values_hbm, r.values), (grad_hbm, r.grad),
            (bias_hbm, r.bias), (rate_hbm, r.rate), (gain_hbm, r.gain),
        ))
    ]
    for i in (0, 1, 2, 5, 6, 7, 3, 4):
        loads[i].start()

    barrier = pltpu.get_barrier_semaphore()
    for k in range(levels):
        pl.semaphore_signal(barrier, inc=1, device_id={"seq": partners[k]}, device_id_type=mesh_id)
    if zrows > 1:
        @pl.when(row < zrows - 1)
        def _():
            pl.semaphore_signal(barrier, inc=1, device_id={"seq": up_row}, device_id_type=mesh_id)

        @pl.when(row > 0)
        def _():
            pl.semaphore_signal(barrier, inc=1, device_id={"seq": down_row}, device_id_type=mesh_id)

    r.hot[...] = one_hot(TILE, head_size, width)
    r.hot3[...] = one_hot_stacked(heads, head_size, width)
    loads[0].wait()
    loads[1].wait()
    layer = r.layer[...]
    proj = mm(layer, r.wbc[...]).astype(BF16)
    r.proj[...] = proj
    r.proj_t[...] = proj.T
    for i in (2, 5, 6, 7):
        loads[i].wait()
    raw = mm_nt(layer, r.wdt[...]) + r.bias[...]
    r.raw[...] = raw
    step = jnp.maximum(raw, 0.0) + jnp.log1p(jnp.exp(-jnp.abs(raw)))
    r.step[...] = step
    decay = -jnp.exp(r.rate[...]) * step
    run = exact_mm(triangle(tokens, lambda a, b: a >= b), decay)
    r.run[...] = run
    total = run[tokens - 1 :, :]
    r.step3[...] = stacked(step)
    r.tail3[...] = stacked(jnp.exp(total - run))
    r.tots[0] = jnp.zeros((8, TILE), F32)
    r.tots[0, :, :heads] = jnp.broadcast_to(total, (8, heads))
    if zrows > 1:
        count = levels + jnp.where(row < zrows - 1, 1, 0) + jnp.where(row > 0, 1, 0)
    else:
        count = levels
    pl.semaphore_wait(barrier, count)

    def remote(source, target, send, receive, device):
        return pltpu.make_async_remote_copy(
            src_ref=source, dst_ref=target, send_sem=send, recv_sem=receive,
            device_id={"seq": device}, device_id_type=mesh_id,
        )

    def tot_copy(k):
        return remote(r.tots.at[k], r.tot_gets.at[k], r.tot_sems.at[0, k], r.tot_sems.at[1, k],
                      partners[k])

    tot_copy(0).start()

    kinds = ("s", "g")

    def cols_of(k):
        return slice(k * span, (k + 1) * span)

    def at(name, kind):
        return getattr(r, name + "_" + kind)

    def rows_at(which, size):
        return pl.ds(pl.multiple_of(which * size, 8), size)

    def copy(stage, kind, k):
        cols = cols_of(k)
        if stage == 0:
            source = at("st", kind).at[rows_at(1 - bits[0], half), cols]
            target, device = at("get0", kind).at[:, cols], partners[0]
        elif stage == 1:
            source = at("agg1", kind).at[rows_at(1 - bits[1], quarter), cols]
            target, device = at("get1", kind).at[:, cols], partners[1]
        elif stage == 2:
            source, target = at("zout", kind).at[:, cols], at("zin", kind).at[:, cols]
            device = up_row if kind == "s" else down_row
        elif stage == 3:
            source = at("send1", kind).at[:, cols]
            target, device = at("chip", kind).at[rows_at(bits[1], quarter), cols], partners[1]
        else:
            source = at("send0", kind).at[:, cols]
            target, device = at("end", kind).at[rows_at(bits[0], half), cols], partners[0]
        i = kinds.index(kind)
        return remote(source, target, r.comm.at[0, stage, i, k], r.comm.at[1, stage, i, k], device)

    def tot_done(k):
        tot_copy(k).wait_recv()
        mine, other = r.tots[k], r.tot_gets[k]
        both = jnp.concatenate([mine, other], axis=0)
        stacked = jnp.concatenate(list(three_way(both)), axis=0)
        wide = mm(stacked, r.hot[...])
        wide = jnp.exp(wide[0:16] + wide[16:32] + wide[32:48])
        r.decays[2 * k] = wide[0:8]
        r.decays[2 * k + 1] = wide[8:16]
        if k == 0:
            r.tots[1] = mine + other
            tot_copy(1).start()
        else:
            r.decays[4] = wide[0:8] * wide[8:16]

    first0, first1 = bits[0] == 0, bits[1] == 0

    def make_states(kind, block):
        if block == 0:
            loads[3 if kind == "s" else 4].wait()
        cols = slice(block * BLOCK * span, (block + 1) * BLOCK * span)
        hot = r.hot3[:, cols]
        if kind == "s":
            step_w = mm(r.step3[...], hot)
            r.step_w[:, cols] = step_w
            tail_w = mm(r.tail3[...], hot)
            r.tail_w[:, cols] = tail_w
            u = step_w * r.values[:, cols].astype(F32)
            r.u[:, cols] = u.astype(BF16)
            tsv = (tail_w * u).astype(BF16)
            r.tsv[:, cols] = tsv
            r.st_s[:, cols] = mm(r.proj_t[:state_dim], tsv)
        else:
            if block == 0:
                r.lead3[...] = stacked(jnp.exp(r.run[...]))
            lead_w = mm(r.lead3[...], hot)
            r.lead_w[:, cols] = lead_w
            lg = (lead_w * r.grad[:, cols].astype(F32)).astype(BF16)
            r.lg[:, cols] = lg
            r.st_g[:, cols] = mm(r.proj_t[state_dim:], lg)
        for k in range(block * BLOCK, (block + 1) * BLOCK):
            copy(0, kind, k).start()

    def merge(kind, first, mine, got, e_mine, e_other):
        if kind == "s":
            return jnp.where(first, e_other * mine + got, mine + e_mine * got)
        return jnp.where(first, mine + e_mine * got, e_other * mine + got)

    def split(kind, first, parent, mine, got, e_mine, e_other):
        far, near = e_other * parent + got, e_mine * parent + mine
        if kind == "s":
            return jnp.where(first, parent, far), jnp.where(first, near, parent)
        return jnp.where(first, far, parent), jnp.where(first, parent, near)

    def pair_up(kind, k):
        copy(0, kind, k).wait_recv()
        cols = cols_of(k)
        mine = at("st", kind)[rows_at(bits[0], half), cols]
        got = at("get0", kind)[:, cols]
        at("agg1", kind)[:, cols] = merge(
            kind, first0, mine, got, r.decays[0, 0:1, cols], r.decays[1, 0:1, cols])
        copy(1, kind, k).start()

    def row_up(kind, k):
        copy(1, kind, k).wait_recv()
        cols = cols_of(k)
        mine = at("agg1", kind)[rows_at(bits[1], quarter), cols]
        got = at("get1", kind)[:, cols]
        at("agg2", kind)[:, cols] = merge(
            kind, first1, mine, got, r.decays[2, 0:1, cols], r.decays[3, 0:1, cols])

    def chain(kind, k, place):
        cols = cols_of(k)
        if place > 0:
            copy(2, kind, k).wait_recv()
            parent = at("zin", kind)[:, cols]
        else:
            parent = jnp.zeros((quarter, span), F32)
        if place < zrows - 1:
            passed = at("agg2", kind)[:, cols]
            if place > 0:
                passed = r.decays[4, 0:1, cols] * parent + passed
            at("zout", kind)[:, cols] = passed
            copy(2, kind, k).start()
        if place == 0:
            at("zin", kind)[:, cols] = parent

    def row_down(kind, k):
        cols = cols_of(k)
        parent = at("zin", kind)[:, cols]
        mine = at("agg1", kind)[rows_at(bits[1], quarter), cols]
        got = at("get1", kind)[:, cols]
        kept, sent = split(kind, first1, parent, mine, got,
                           r.decays[2, 0:1, cols], r.decays[3, 0:1, cols])
        at("send1", kind)[:, cols] = sent
        copy(3, kind, k).start()
        at("chip", kind)[rows_at(bits[1], quarter), cols] = kept

    def chain_slot(kind, k, place):
        where = place if kind == "s" else zrows - 1 - place
        if zrows == 1:
            chain(kind, k, place)
        else:
            pl.when(row == where)(lambda: chain(kind, k, place))

    def chip_down(kind, k):
        copy(3, kind, k).wait_recv()
        cols = cols_of(k)
        parent = at("chip", kind)[:, cols]
        mine = at("st", kind)[rows_at(bits[0], half), cols]
        got = at("get0", kind)[:, cols]
        kept, sent = split(kind, first0, parent, mine, got,
                           r.decays[0, 0:1, cols], r.decays[1, 0:1, cols])
        at("send0", kind)[:, cols] = sent
        copy(4, kind, k).start()
        at("end", kind)[rows_at(bits[0], half), cols] = kept

    def gather(name, k, x):
        ref = getattr(r, name)
        ref[...] = x if k == 0 else ref[...] + x

    def forward_tail(k):
        copy(4, "s", k).wait_recv()
        cols = cols_of(k)
        hot = r.hot[:heads, cols]
        inc = r.end_s[:, cols].astype(BF16)
        lead_grad = r.lead_w[:, cols] * r.grad[:, cols].astype(F32)
        gather("reads", k, head_sum(lead_grad * mm(r.proj[:, state_dim:], inc), hot))
        gather("gc", k, mm_nt(r.lg[:, cols], inc))

    def inner_tail(k):
        cols = cols_of(k)
        hot = r.hot[:heads, cols]
        gather("cols", k, head_sum(r.u[:, cols].astype(F32) * r.gu[:, cols], hot))
        products = r.values[:, cols].astype(F32) * r.grad[:, cols].astype(F32)
        products = jnp.sum(products, axis=0, keepdims=True)
        gather("skips", k, head_sum(jnp.broadcast_to(products, (8, span)), hot))

    def backward_tail(k):
        copy(4, "g", k).wait_recv()
        cols = cols_of(k)
        hot = r.hot[:heads, cols]
        outgoing = r.end_g[:, cols]
        out = outgoing.astype(BF16)
        values = r.values[:, cols].astype(F32)
        gather("gb", k, mm_nt(r.tsv[:, cols], out))
        back = r.tail_w[:, cols] * mm(r.proj[:, :state_dim], out)
        gather("backs", k, head_sum(values * back, hot))
        gu = r.gu[:, cols] + back
        gather("gsteps", k, head_sum(values * gu, hot))
        cross = jnp.sum(r.end_s[:, cols] * outgoing, axis=0, keepdims=True)
        gather("cross", k, head_sum(jnp.broadcast_to(cross, (8, span)), hot))
        gain = mm(stacked(jnp.broadcast_to(r.gain[...], (8, heads))), r.hot3[:, cols])[0:1]
        gvalues_ref[:, cols] = (
            r.step_w[:, cols] * gu + gain * r.grad[:, cols].astype(F32)
        ).astype(BF16)

    plan = reduce_plan(depth, devices, heads)
    share, lanes, group = packing(depth, devices, heads)

    def places(order):
        return [
            sum(((shard >> order[i]) & 1) * (devices >> (i + 1)) for i in range(levels))
            for shard in range(devices)
        ]

    def offset(order, count):
        result = 0
        for i in range(count):
            result = result + bits[order[i]] * (devices >> (i + 1))
        return result

    def part(q, i, which):
        size, order = plan[q][2], plan[q][3]
        start = (offset(order, i) + which * (devices >> (i + 1))) * size
        return pl.ds(pl.multiple_of(start, 8), (devices >> (i + 1)) * size)

    def reduce_copy(q, i):
        k = plan[q][3][i]
        return remote(
            getattr(r, f"sum{q}").at[part(q, i, 1 - bits[k])], getattr(r, f"rget{q}_{i}"),
            r.rsem.at[0, i, q], r.rsem.at[1, i, q], partners[k],
        )

    def reduce_step(q, i):
        k = plan[q][3][i]
        reduce_copy(q, i).wait_recv()
        sums = getattr(r, f"sum{q}")
        mine = part(q, i, bits[k])
        sums[mine] = sums[mine] + getattr(r, f"rget{q}_{i}")[...]
        if i + 1 < levels:
            reduce_copy(q, i + 1).start()

    def send_piece(q):
        plane, first, size, order = plan[q]
        grad = r.gproj[:, plane * state_dim : (plane + 1) * state_dim]
        sums = getattr(r, f"sum{q}")
        where = places(order)
        product = mm(r.layer_t[devices * first : devices * (first + size)], grad)
        for shard in range(devices):
            sums[where[shard] * size : (where[shard] + 1) * size] = (
                product[shard * size : (shard + 1) * size])
        reduce_copy(q, 0).start()

    def finish_c():
        grad_c = r.gc[...] + mm_tn(r.gscores[...].astype(BF16), r.proj[:, :state_dim])
        grad_c = grad_c.astype(BF16)
        r.gproj[:, state_dim : 2 * state_dim] = grad_c

    def finish_b():
        grad_b = r.gb[...] + mm(r.gscores[...].astype(BF16), r.proj[:, state_dim:])
        grad_b = grad_b.astype(BF16)
        r.gproj[:, :state_dim] = grad_b

    def before_dt():
        upper = triangle(tokens, lambda a, b: a <= b)
        inner = r.rows[:, 0, :].T + r.reads[...] - r.cols[...]
        r.pre[...] = exact_mm(upper, inner)
        r.sigmoid[...] = 1.0 / (1.0 + jnp.exp(-r.raw[...]))

    def finish_dt():
        step = r.step[...]
        rate = jnp.exp(r.rate[...])
        total = r.run[tokens - 1 :, :]
        lower = triangle(tokens, lambda a, b: a > b)
        grad_decay = (
            r.pre[...] + exact_mm(lower, step * r.backs[...]) + jnp.exp(total) * r.cross[0:1]
        )
        grad_raw = (r.gsteps[...] - rate * grad_decay) * r.sigmoid[...]
        r.gproj[:, 2 * state_dim :] = grad_raw.astype(BF16)
        small = jnp.concatenate([
            jnp.sum(grad_raw, axis=0, keepdims=True),
            -rate * jnp.sum(grad_decay * step, axis=0, keepdims=True),
            r.skips[0:1],
            jnp.zeros((5, heads), F32),
        ], axis=0)
        r.small[...] = jnp.concatenate([small, jnp.zeros((8, TILE - heads), F32)], axis=1)

    def send_dt():
        narrow = r.gproj[:, 2 * state_dim :]
        product = mm(r.layer_t[...], jnp.concatenate(
            [narrow.astype(F32), jnp.zeros((tokens, TILE - heads), F32)], axis=1).astype(BF16))
        small = r.small[...]

        def shard_rows(shard, begin, count):
            found, first = [], 0
            for size in pieces_of(share):
                low, high = max(begin, first), min(begin + count, first + size)
                if low < high:
                    base = devices * first + shard * size - first
                    found.append(product[base + low : base + high])
                first += size
            return found[0] if len(found) == 1 else jnp.concatenate(found, axis=0)

        q = len(plan) - 1
        unit = group + 8
        sums = getattr(r, f"sum{q}")
        where = places(plan[q][3])
        for shard in range(devices):
            start = where[shard] * unit
            packed = jnp.zeros((group, TILE), F32)
            for j in range(lanes):
                count = min(share - j * group, group)
                if count <= 0:
                    continue
                piece = shard_rows(shard, j * group, count)
                if j > 0:
                    piece = pltpu.roll(piece, j * heads, 1)
                if count < group:
                    piece = jnp.concatenate(
                        [piece, jnp.zeros((group - count, TILE), F32)], axis=0)
                packed = packed + piece
            sums[start : start + group] = packed
            sums[start + group : start + unit] = small
        reduce_copy(q, 0).start()

    def layer_tail():
        glayer_ref[...] = (
            mm_nt(r.gproj[:, : 2 * state_dim], r.wbc[...])
            + mm(r.gproj[:, 2 * state_dim :], r.wdt[...])
        ).astype(BF16)

    def prepare():
        run = r.run[...]
        run_rows = run.T
        for head in range(heads):
            r.run_rows[head] = run_rows[head : head + 1]
        r.parts[...] = stacked(run)
        r.scores[...] = mm_nt(r.proj[:, :state_dim], r.proj[:, state_dim:])
        r.gscores[...] = jnp.zeros_like(r.gscores)

    def turn():
        turned = r.layer[...].T
        first = 0
        for size in pieces_of(share):
            for shard in range(devices):
                start, target = shard * share + first, devices * first + shard * size
                r.layer_t[target : target + size] = turned[start : start + size]
            first += size

    def body(pair, _):
        inner_pair(pair, heads, r.u, r.grad, r.scores, r.parts, r.run_rows,
                   r.gu, r.rows, r.gscores, head_size)
        return 0

    events = []

    def event(time, cost, work, *args):
        events.append((time, len(events), cost, functools.partial(work, *args)))

    n = CHUNKS
    wire, flight, near, hop = 7.05 / n, 3.0, 1.05, 2.9 + 7.2 / n
    start, blocks = 3.9, n // BLOCK
    make_s, make_g = 2.25 / blocks, 1.95 / blocks
    first = start + make_s + near
    event(start + 2 * make_s - 0.01, 0.27, tot_done, 0)
    event(first + 2.2, 0.25, tot_done, 1)
    for block in range(blocks):
        event(start + make_s * block, make_s, make_states, "s", block)
        event(start + make_s * blocks + make_g * block, make_g, make_states, "g", block)
    for k in range(n):
        block = k // BLOCK
        event(start + make_s * (block + 1) + near, 0.02, pair_up, "s", k)
        event(start + make_s * blocks + make_g * (block + 1) + near + 0.3, 0.02, pair_up, "g", k)
        for i, kind in enumerate(kinds):
            arrive = first + wire * (i * n + k + 1) + flight
            event(arrive, 0.02, row_up, kind, k)
            for place in range(zrows):
                event(arrive + hop * min(place, 3) + 0.01, 0.02, chain_slot, kind, k, place)
            down = max(first + wire * (2 + i) * n, first + wire * (i * n + 1) + flight + 3 * hop)
            down = down + wire * k
            event(max(arrive + 3 * hop, down - 1.0) + 0.02, 0.02, row_down, kind, k)
            event(down + wire + flight, 0.02, chip_down, kind, k)
            arrive = down + wire + flight + near
            if kind == "s":
                event(arrive + 0.4, 3.4 / n, forward_tail, k)
            else:
                event(arrive + 0.2, 5.0 / n, backward_tail, k)
            if k == n - 1 and kind == "s":
                c_time = arrive + 0.5
                event(c_time, 0.2, finish_c)
            elif k == n - 1:
                b_time = arrive + 0.3
                event(b_time, 0.2, finish_b)
                event(b_time + 1.5, 0.4, finish_dt)
                event(b_time + 2.0, 0.8, send_dt)
                event(b_time + 5.0, 1.4, layer_tail)
    free = {"z": 0.0, "m": 0.0, "y": first + 4 * n * wire}
    clocks = []
    for q, (plane, offset_rows, size, order) in enumerate(plan):
        piece = q % len(pieces_of(share))
        if plane == 1:
            made = c_time + 0.2 + 0.5 * piece
        elif plane == 0:
            made = b_time + 0.2 + 0.3 * piece
        else:
            made = b_time + 2.5
        if plane < 2:
            event(made, 0.3, send_piece, q)
        ready = made + 0.3 + 1.1
        if plane == 1 and order[1] == 1:
            ready = max(ready, down + 0.1)
        clocks.append([ready, size * 0.045])
        event(clocks[q][0], 0.04, reduce_step, q, 0)
    pending = [(clocks[q][0], q, 1) for q in range(len(plan))]
    while pending:
        pending.sort()
        ready, q, i = pending.pop(0)
        level = plan[q][3][i]
        pace = clocks[q][1]
        clocks[q][1] = pace / 2
        begin = max(ready, free["y" if level == 1 else "z"])
        if level == 1:
            free["y"] = begin + pace
            done_at = begin + pace + 2.8
        elif level == 2:
            free["z"] = begin + pace
            done_at = begin + pace + 2.8
        else:
            free["z"] = begin + pace
            free["m"] = max(begin, free["m"]) + 2 * pace
            done_at = free["m"] + 3.5
        event(done_at, 0.03, reduce_step, q, i)
        if i + 1 < levels:
            pending.append((done_at, q, i + 1))
    events.sort(key=lambda item: item[:2])

    pairs = width // TILE
    soft = [(0.25, prepare)] + [(0.46, None)] * pairs + [(0.4, turn)]
    soft += [(1.7 / n, functools.partial(inner_tail, k)) for k in range(n)]
    state = [0, 0.0, 0]

    def fill(limit):
        count = 0
        while soft and state[1] + soft[0][0] <= limit:
            cost, work = soft.pop(0)
            state[1] += cost
            if work is None:
                count += 1
                continue
            if count:
                lax.fori_loop(state[0], state[0] + count, body, 0)
                state[0], count = state[0] + count, 0
            work()
        if count:
            lax.fori_loop(state[0], state[0] + count, body, 0)
            state[0] += count

    whole = 1e9
    begun = False
    for time, index, cost, work in events:
        if begun:
            fill(whole if work.func in (finish_c, backward_tail) else time + 0.4)
        if work.func is finish_b:
            before_dt()
        work()
        state[1] = max(state[1], time) + cost
        if work.func is pair_up and work.args == ("g", n - 1):
            begun = True

    for q, (plane, first, size, order) in enumerate(plan):
        unit = size
        start = pl.multiple_of(offset(order, levels) * unit, 8)
        result = getattr(r, f"sum{q}")[pl.ds(start, unit)]
        if plane < 2:
            gbc_ref[first : first + size, plane * TILE : (plane + 1) * TILE] = result
        else:
            last_ref[...] = result
    for k in range(2):
        tot_copy(k).wait_send()
    for kind in kinds:
        for k in range(n):
            for stage in (0, 1, 3, 4):
                copy(stage, kind, k).wait_send()
        if zrows > 1:
            sends = row < zrows - 1 if kind == "s" else row > 0

            @pl.when(sends)
            def _(kind=kind):
                for k in range(n):
                    copy(2, kind, k).wait_send()
    for q in range(len(plan)):
        for i in range(levels):
            reduce_copy(q, i).wait_send()


def finish_kernel(heads, group, lanes, gvalues_in, glayer_in, gbc_in, last_in,
                  gvalues_ref, glayer_ref, gbc_ref, gdt_ref, gbias_ref, grate_ref, gskip_ref, sems):
    copies = [
        pltpu.make_async_copy(source, target, sems.at[i])
        for i, (source, target) in enumerate((
            (gvalues_in, gvalues_ref), (glayer_in, glayer_ref), (gbc_in, gbc_ref),
        ))
    ]
    for copy in copies:
        copy.start()
    last = last_in[...]
    share = gdt_ref.shape[1]
    pieces = []
    for j in range(lanes):
        count = min(share - j * group, group)
        if count > 0:
            pieces.append(last[:count, j * heads : (j + 1) * heads])
    gdt_ref[...] = jnp.concatenate(pieces, axis=0).T
    gbias_ref[...] = last[group : group + 1, :heads]
    grate_ref[...] = last[group + 1 : group + 2, :heads]
    gskip_ref[...] = last[group + 2 : group + 3, :heads]
    for copy in copies:
        copy.wait()


def local(layer_in, ssm_in, weight_bc, weight_dt, bias_dt, log_rate, skip_gain, grad_out):
    tokens, depth = layer_in.shape
    heads = log_rate.shape[0]
    width = ssm_in.shape[1]
    state_dim = weight_bc.shape[1] // 2
    devices = lax.axis_size("seq")
    share, lanes, group = packing(depth, devices, heads)
    scratch = scratch_list(tokens, depth, width, heads, state_dim, devices)
    shape = jax.ShapeDtypeStruct
    gvalues, glayer, gbc, last = pl.pallas_call(
        functools.partial(mega_kernel, devices, list(scratch)),
        out_shape=[
            pltpu.VMEM((tokens, width), BF16),
            pltpu.VMEM((tokens, depth), BF16),
            pltpu.VMEM((share, 2 * state_dim), F32),
            pltpu.VMEM((group + 8, TILE), F32),
        ],
        in_specs=[ANY] * 8,
        out_specs=[VMEM, VMEM, VMEM, VMEM],
        scratch_shapes=list(scratch.values()),
        compiler_params=pltpu.CompilerParams(
            collective_id=0, has_side_effects=True, vmem_limit_bytes=VMEM_LIMIT
        ),
        name="mixer",
    )(layer_in, ssm_in, weight_bc, weight_dt.T, bias_dt[None, :], log_rate[None, :],
      skip_gain[None, :], grad_out)
    outs = pl.pallas_call(
        functools.partial(finish_kernel, heads, group, lanes),
        out_shape=[
            shape((tokens, width), BF16),
            shape((tokens, depth), BF16),
            shape((share, 2 * state_dim), F32),
            shape((heads, share), F32),
            shape((1, heads), F32),
            shape((1, heads), F32),
            shape((1, heads), F32),
        ],
        in_specs=[VMEM] * 4,
        out_specs=[ANY] * 3 + [VMEM] * 4,
        scratch_shapes=[pltpu.SemaphoreType.DMA((3,))],
        compiler_params=pltpu.CompilerParams(vmem_limit_bytes=8 * 1024 * 1024),
        name="finish",
    )(gvalues, glayer, gbc, last)
    return tuple(outs[:3]) + (outs[3].T,) + tuple(out[0] for out in outs[4:])


def solution(mesh):
    rows = P(("groups", "seq"), None)
    in_specs = (rows, rows, P(), P(), P(), P(), P(), rows)
    out_specs = (rows, rows, rows, rows, P("groups"), P("groups"), P("groups"))
    return jax.shard_map(local, mesh=mesh, in_specs=in_specs, out_specs=out_specs, check_vma=False)
```

```python
import functools
import jax
import jax.numpy as jnp
from jax import lax
from jax.experimental import pallas as pl
from jax.experimental.pallas import tpu as pltpu
from jax.sharding import PartitionSpec as P

F32 = jnp.float32
BF16 = jnp.bfloat16
TILE = 128
CHUNKS = 10
BLOCK = 2
TAILS = 4
LOADS = 4
REDUCE_C, REDUCE_B, REDUCE_DT = "zzyy", "yyyz", "z"
VMEM_LIMIT = 52 * 1024 * 1024
VMEM = pl.BlockSpec(memory_space=pltpu.VMEM)
ANY = pl.BlockSpec(memory_space=pl.ANY)


def mm(left, right):
    return lax.dot_general(left, right, (((1,), (0,)), ((), ())), preferred_element_type=F32)


def mm_nt(left, right):
    return lax.dot_general(left, right, (((1,), (1,)), ((), ())), preferred_element_type=F32)


def mm_tn(left, right):
    return lax.dot_general(left, right, (((0,), (0,)), ((), ())), preferred_element_type=F32)


def three_way(x):
    high = x.astype(BF16)
    rest = x - high.astype(F32)
    middle = rest.astype(BF16)
    return high, middle, (rest - middle.astype(F32)).astype(BF16)


def one_hot(heads, width, columns, first=0):
    row = lax.broadcasted_iota(jnp.int32, (heads, columns), 0)
    col = lax.broadcasted_iota(jnp.int32, (heads, columns), 1) + first
    inside = (col >= row * width) & (col < (row + 1) * width)
    return jnp.where(inside, 1.0, 0.0).astype(BF16)


def one_hot_stacked(heads, width, columns, first=0):
    row = lax.rem(lax.broadcasted_iota(jnp.int32, (TILE, columns), 0), heads)
    real = lax.broadcasted_iota(jnp.int32, (TILE, columns), 0) < 3 * heads
    col = lax.broadcasted_iota(jnp.int32, (TILE, columns), 1) + first
    inside = (col >= row * width) & (col < (row + 1) * width) & real
    return jnp.where(inside, 1.0, 0.0).astype(BF16)


def stacked(x):
    rows, heads = x.shape
    zero = jnp.zeros((rows, TILE - heads), F32)
    result = None
    for i, piece in enumerate(three_way(x)):
        piece = jnp.concatenate([piece.astype(F32), zero], axis=1)
        piece = piece if i == 0 else pltpu.roll(piece, i * heads, 1)
        result = piece if i == 0 else result + piece
    return result.astype(BF16)


def head_sum(x, hot):
    high = x.astype(BF16)
    low = (x - high.astype(F32)).astype(BF16)
    return mm_nt(high, hot) + mm_nt(low, hot)


def exact_mm(mask, x):
    parts = three_way(x)
    return mm(mask, parts[0]) + mm(mask, parts[1]) + mm(mask, parts[2])


def triangle(size, compare):
    row = lax.broadcasted_iota(jnp.int32, (size, size), 0)
    col = lax.broadcasted_iota(jnp.int32, (size, size), 1)
    return jnp.where(compare(row, col), 1.0, 0.0).astype(BF16)


def inner_pair(pair, heads, u_ref, grad_ref, scores_ref, parts_ref, run_rows_ref,
               gu_ref, rows_ref, gscores_ref, head_size):
    tokens = u_ref.shape[0]
    blocks = tokens // TILE
    per = TILE // head_size
    cols = pl.ds(pl.multiple_of(pair * TILE, TILE), TILE)
    lane = lax.broadcasted_iota(jnp.int32, (TILE, TILE), 1)
    causal = lax.broadcasted_iota(jnp.int32, (TILE, TILE), 0) <= lane
    wide = one_hot_stacked(heads, TILE, per * TILE, pair * (per * TILE))
    run_cols = mm(parts_ref[...], wide)
    grads = [grad_ref[t * TILE : (t + 1) * TILE, cols] for t in range(blocks)]
    gus = [jnp.zeros((TILE, TILE), F32) for _ in range(blocks)]
    for sub in range(per):
        head = pair * per + sub
        keep = (lane >= sub * head_size) & (lane < (sub + 1) * head_size)
        rows = [jnp.zeros((1, TILE), F32) for _ in range(blocks)]
        for s in range(blocks):
            srange = slice(s * TILE, (s + 1) * TILE)
            run_col = run_cols[srange, sub * TILE : (sub + 1) * TILE]
            u_head = jnp.where(keep, u_ref[srange, cols], jnp.zeros((), BF16))
            gu = jnp.zeros((TILE, TILE), F32)
            for t in range(s, blocks):
                trange = slice(t * TILE, (t + 1) * TILE)
                gap = run_rows_ref[head, :, trange] - run_col
                if s == t:
                    gap = jnp.where(causal, gap, -jnp.inf)
                factor = jnp.exp(gap)
                mixing = (factor * scores_ref[srange, trange]).astype(BF16)
                weight = mm_nt(u_head, grads[t])
                gscores_ref[srange, trange] += factor * weight
                rows[t] += jnp.sum(mixing.astype(F32) * weight, axis=0, keepdims=True)
                gu += mm(mixing, grads[t])
            gus[s] = jnp.where(keep, gu, gus[s])
        for t in range(blocks):
            rows_ref[head, :, t * TILE : (t + 1) * TILE] = rows[t]
    for s in range(blocks):
        gu_ref[s * TILE : (s + 1) * TILE, cols] = gus[s]


def packing(depth, devices, heads):
    share = depth // devices
    lanes = TILE // heads
    group = -(-share // (8 * lanes)) * 8
    return share, lanes, group


def pieces_of(share):
    units = share // 16
    if share % 16 or units < 4:
        return [share]
    return [16 * ((units + 3 - i) // 4) for i in range(4)]


def reduce_plan(depth, devices, heads):
    share, lanes, group = packing(depth, devices, heads)
    levels = devices.bit_length() - 1
    y_first = list(range(levels))
    z_first = [0] + list(range(2, levels)) + [1]
    plan, first = [], 0
    cuts = pieces_of(share)
    for plane, names in ((1, REDUCE_C), (0, REDUCE_B)):
        first = 0
        for piece, size in enumerate(cuts):
            plan.append((plane, first, size, y_first if names[piece] == "y" else z_first))
            first += size
    plan.append((2, 0, group + 8, y_first if REDUCE_DT == "y" else z_first))
    return plan


def scratch_list(tokens, depth, width, heads, state_dim, devices):
    levels = devices.bit_length() - 1
    half, quarter = state_dim // 2, state_dim // 4
    plan = reduce_plan(depth, devices, heads)
    names = {}

    def add(name, shape, dtype=F32):
        names[name] = pltpu.VMEM(shape, dtype)

    add("layer", (tokens, depth), BF16)
    add("values", (tokens, width), BF16)
    add("grad", (tokens, width), BF16)
    add("wbc", (depth, 2 * state_dim), BF16)
    add("wdt", (heads, depth), BF16)
    add("layer_t", (depth, tokens), BF16)
    add("proj", (tokens, 2 * state_dim), BF16)
    add("proj_t", (2 * state_dim, tokens), BF16)
    add("hot", (TILE, width), BF16)
    for name in ("parts", "step3", "tail3", "lead3"):
        add(name, (tokens, TILE), BF16)
    add("hot3", (TILE, width), BF16)
    for name in ("bias", "rate", "gain"):
        add(name, (1, heads))
    add("pre", (tokens, heads))
    add("sigmoid", (tokens, heads))
    for name in ("raw", "step", "run"):
        add(name, (tokens, heads))
    add("run_rows", (heads, 1, tokens))
    add("rows", (heads, 1, tokens))
    add("scores", (tokens, tokens))
    add("gscores", (tokens, tokens))
    for name in ("step_w", "lead_w", "tail_w", "gu"):
        add(name, (tokens, width))
    for name in ("u", "tsv", "lg"):
        add(name, (tokens, width), BF16)
    for name in ("reads", "cols", "backs", "gsteps"):
        add(name, (tokens, heads))
    add("cross", (8, heads))
    add("skips", (8, heads))
    add("small", (8, TILE))
    add("gc", (tokens, state_dim))
    add("gb", (tokens, state_dim))
    add("gproj", (tokens, 2 * state_dim + heads), BF16)
    for kind in ("s", "g"):
        add("st_" + kind, (state_dim, width))
        add("get0_" + kind, (half, width))
        add("agg1_" + kind, (half, width))
        add("get1_" + kind, (quarter, width))
        add("agg2_" + kind, (quarter, width))
        add("zin_" + kind, (quarter, width))
        add("zout_" + kind, (quarter, width))
        add("send1_" + kind, (quarter, width))
        add("chip_" + kind, (half, width))
        add("send0_" + kind, (half, width))
        add("end_" + kind, (state_dim, width))
    add("tots", (2, 8, TILE))
    add("tot_gets", (2, 8, TILE))
    add("decays", (5, 8, width))
    for q, (plane, first, size, order) in enumerate(plan):
        add(f"sum{q}", (devices * size, TILE))
        for i in range(levels):
            add(f"rget{q}_{i}", ((devices >> (i + 1)) * size, TILE))
    add_sem = lambda name, shape: names.__setitem__(name, pltpu.SemaphoreType.DMA(shape))
    add_sem("load", (6,))
    add_sem("early", (2, LOADS))
    add_sem("comm", (2, 5, 2, CHUNKS))
    add_sem("tot_sems", (2, 2))
    add_sem("rsem", (2, levels, len(plan)))
    return names


class Box:
    pass


def mega_kernel(devices, names, layer_hbm, values_hbm, wbc_hbm, wdt_hbm, bias_hbm, rate_hbm,
                gain_hbm, grad_hbm, gvalues_ref, glayer_ref, gbc_ref, last_ref, *refs):
    r = Box()
    for name, ref in zip(names, refs):
        setattr(r, name, ref)
    tokens, depth = r.layer.shape
    width = r.values.shape[1]
    heads = r.bias.shape[1]
    head_size = width // heads
    state_dim = r.st_s.shape[0]
    half, quarter = state_dim // 2, state_dim // 4
    levels = devices.bit_length() - 1
    zrows = devices // 4
    span = width // CHUNKS
    me = lax.axis_index("seq")
    bits = [lax.rem(me // (1 << k), 2) for k in range(levels)]
    partners = [me + (1 - 2 * bits[k]) * (1 << k) for k in range(levels)]
    row = me // 4
    up_row = lax.rem(me + 4, devices)
    down_row = lax.rem(me + devices - 4, devices)
    mesh_id = pl.DeviceIdType.MESH

    pieces = [slice(i * depth // LOADS, (i + 1) * depth // LOADS) for i in range(LOADS)]
    early = [
        [
            pltpu.make_async_copy(source, target, r.early.at[j, i])
            for j, (source, target) in enumerate((
                (layer_hbm.at[:, piece], r.layer.at[:, piece]),
                (wbc_hbm.at[piece], r.wbc.at[piece]),
            ))
        ]
        for i, piece in enumerate(pieces)
    ]
    loads = [
        pltpu.make_async_copy(source, target, r.load.at[i])
        for i, (source, target) in enumerate((
            (wdt_hbm, r.wdt), (bias_hbm, r.bias), (rate_hbm, r.rate), (gain_hbm, r.gain),
            (values_hbm, r.values), (grad_hbm, r.grad),
        ))
    ]
    for i in range(4):
        loads[i].start()
    for group in early:
        for load in group:
            load.start()
    for i in (4, 5):
        loads[i].start()

    barrier = pltpu.get_barrier_semaphore()
    for k in range(levels):
        pl.semaphore_signal(barrier, inc=1, device_id={"seq": partners[k]}, device_id_type=mesh_id)
    if zrows > 1:
        @pl.when(row < zrows - 1)
        def _():
            pl.semaphore_signal(barrier, inc=1, device_id={"seq": up_row}, device_id_type=mesh_id)

        @pl.when(row > 0)
        def _():
            pl.semaphore_signal(barrier, inc=1, device_id={"seq": down_row}, device_id_type=mesh_id)

    r.hot[...] = one_hot(TILE, head_size, width)
    r.hot3[...] = one_hot_stacked(heads, head_size, width)
    for i in range(4):
        loads[i].wait()
    proj, raw = None, None
    for piece, group in zip(pieces, early):
        for load in group:
            load.wait()
        layer = r.layer[:, piece]
        add_raw = mm_nt(layer, r.wdt[:, piece])
        add_proj = mm(layer, r.wbc[piece])
        proj = add_proj if proj is None else proj + add_proj
        raw = add_raw if raw is None else raw + add_raw
    raw = raw + r.bias[...]
    r.raw[...] = raw
    proj = proj.astype(BF16)
    r.proj[...] = proj
    r.proj_t[...] = proj.T
    step = jnp.maximum(raw, 0.0) + jnp.log1p(jnp.exp(-jnp.abs(raw)))
    r.step[...] = step
    decay = -jnp.exp(r.rate[...]) * step
    run = exact_mm(triangle(tokens, lambda a, b: a >= b), decay)
    r.run[...] = run
    total = run[tokens - 1 :, :]
    r.step3[...] = stacked(step)
    r.tail3[...] = stacked(jnp.exp(total - run))
    r.tots[0] = jnp.zeros((8, TILE), F32)
    r.tots[0, :, :heads] = jnp.broadcast_to(total, (8, heads))
    if zrows > 1:
        count = levels + jnp.where(row < zrows - 1, 1, 0) + jnp.where(row > 0, 1, 0)
    else:
        count = levels
    pl.semaphore_wait(barrier, count)

    def remote(source, target, send, receive, device):
        return pltpu.make_async_remote_copy(
            src_ref=source, dst_ref=target, send_sem=send, recv_sem=receive,
            device_id={"seq": device}, device_id_type=mesh_id,
        )

    def tot_copy(k):
        return remote(r.tots.at[k], r.tot_gets.at[k], r.tot_sems.at[0, k], r.tot_sems.at[1, k],
                      partners[k])

    tot_copy(0).start()

    kinds = ("s", "g")

    def cols_of(k):
        return slice(k * span, (k + 1) * span)

    def at(name, kind):
        return getattr(r, name + "_" + kind)

    def rows_at(which, size):
        return pl.ds(pl.multiple_of(which * size, 8), size)

    def copy(stage, kind, k):
        cols = cols_of(k)
        if stage == 0:
            source = at("st", kind).at[rows_at(1 - bits[0], half), cols]
            target, device = at("get0", kind).at[:, cols], partners[0]
        elif stage == 1:
            source = at("agg1", kind).at[rows_at(1 - bits[1], quarter), cols]
            target, device = at("get1", kind).at[:, cols], partners[1]
        elif stage == 2:
            source, target = at("zout", kind).at[:, cols], at("zin", kind).at[:, cols]
            device = up_row if kind == "s" else down_row
        elif stage == 3:
            source = at("send1", kind).at[:, cols]
            target, device = at("chip", kind).at[rows_at(bits[1], quarter), cols], partners[1]
        else:
            source = at("send0", kind).at[:, cols]
            target, device = at("end", kind).at[rows_at(bits[0], half), cols], partners[0]
        i = kinds.index(kind)
        return remote(source, target, r.comm.at[0, stage, i, k], r.comm.at[1, stage, i, k], device)

    def tot_done(k):
        tot_copy(k).wait_recv()
        mine, other = r.tots[k], r.tot_gets[k]
        both = jnp.concatenate([mine, other], axis=0)
        stacked = jnp.concatenate(list(three_way(both)), axis=0)
        wide = mm(stacked, r.hot[...])
        wide = jnp.exp(wide[0:16] + wide[16:32] + wide[32:48])
        r.decays[2 * k] = wide[0:8]
        r.decays[2 * k + 1] = wide[8:16]
        if k == 0:
            r.tots[1] = mine + other
            tot_copy(1).start()
        else:
            r.decays[4] = wide[0:8] * wide[8:16]

    first0, first1 = bits[0] == 0, bits[1] == 0

    def make_states(kind, block):
        if block == 0:
            loads[4 if kind == "s" else 5].wait()
        cols = slice(block * BLOCK * span, (block + 1) * BLOCK * span)
        hot = r.hot3[:, cols]
        if kind == "s":
            step_w = mm(r.step3[...], hot)
            r.step_w[:, cols] = step_w
            tail_w = mm(r.tail3[...], hot)
            r.tail_w[:, cols] = tail_w
            u = step_w * r.values[:, cols].astype(F32)
            r.u[:, cols] = u.astype(BF16)
            tsv = (tail_w * u).astype(BF16)
            r.tsv[:, cols] = tsv
            r.st_s[:, cols] = mm(r.proj_t[:state_dim], tsv)
        else:
            if block == 0:
                r.lead3[...] = stacked(jnp.exp(r.run[...]))
            lead_w = mm(r.lead3[...], hot)
            r.lead_w[:, cols] = lead_w
            lg = (lead_w * r.grad[:, cols].astype(F32)).astype(BF16)
            r.lg[:, cols] = lg
            r.st_g[:, cols] = mm(r.proj_t[state_dim:], lg)
        for k in range(block * BLOCK, (block + 1) * BLOCK):
            copy(0, kind, k).start()

    def merge(kind, first, mine, got, e_mine, e_other):
        if kind == "s":
            return jnp.where(first, e_other * mine + got, mine + e_mine * got)
        return jnp.where(first, mine + e_mine * got, e_other * mine + got)

    def split(kind, first, parent, mine, got, e_mine, e_other):
        far, near = e_other * parent + got, e_mine * parent + mine
        if kind == "s":
            return jnp.where(first, parent, far), jnp.where(first, near, parent)
        return jnp.where(first, far, parent), jnp.where(first, parent, near)

    def pair_up(kind, k):
        copy(0, kind, k).wait_recv()
        cols = cols_of(k)
        mine = at("st", kind)[rows_at(bits[0], half), cols]
        got = at("get0", kind)[:, cols]
        at("agg1", kind)[:, cols] = merge(
            kind, first0, mine, got, r.decays[0, 0:1, cols], r.decays[1, 0:1, cols])
        copy(1, kind, k).start()

    def row_up(kind, k):
        copy(1, kind, k).wait_recv()
        cols = cols_of(k)
        mine = at("agg1", kind)[rows_at(bits[1], quarter), cols]
        got = at("get1", kind)[:, cols]
        at("agg2", kind)[:, cols] = merge(
            kind, first1, mine, got, r.decays[2, 0:1, cols], r.decays[3, 0:1, cols])

    def chain(kind, k, place):
        cols = cols_of(k)
        if place > 0:
            copy(2, kind, k).wait_recv()
            parent = at("zin", kind)[:, cols]
        else:
            parent = jnp.zeros((quarter, span), F32)
        if place < zrows - 1:
            passed = at("agg2", kind)[:, cols]
            if place > 0:
                passed = r.decays[4, 0:1, cols] * parent + passed
            at("zout", kind)[:, cols] = passed
            copy(2, kind, k).start()
        if place == 0:
            at("zin", kind)[:, cols] = parent

    def row_down(kind, k):
        cols = cols_of(k)
        parent = at("zin", kind)[:, cols]
        mine = at("agg1", kind)[rows_at(bits[1], quarter), cols]
        got = at("get1", kind)[:, cols]
        kept, sent = split(kind, first1, parent, mine, got,
                           r.decays[2, 0:1, cols], r.decays[3, 0:1, cols])
        at("send1", kind)[:, cols] = sent
        copy(3, kind, k).start()
        at("chip", kind)[rows_at(bits[1], quarter), cols] = kept

    def chain_slot(kind, k, place):
        where = place if kind == "s" else zrows - 1 - place
        if zrows == 1:
            chain(kind, k, place)
        else:
            pl.when(row == where)(lambda: chain(kind, k, place))

    def chip_down(kind, k):
        copy(3, kind, k).wait_recv()
        cols = cols_of(k)
        parent = at("chip", kind)[:, cols]
        mine = at("st", kind)[rows_at(bits[0], half), cols]
        got = at("get0", kind)[:, cols]
        kept, sent = split(kind, first0, parent, mine, got,
                           r.decays[0, 0:1, cols], r.decays[1, 0:1, cols])
        at("send0", kind)[:, cols] = sent
        copy(4, kind, k).start()
        at("end", kind)[rows_at(bits[0], half), cols] = kept

    def gather(name, k, x):
        ref = getattr(r, name)
        ref[...] = x if k == 0 else ref[...] + x

    def forward_tail(k):
        copy(4, "s", k).wait_recv()
        cols = cols_of(k)
        hot = r.hot[:heads, cols]
        inc = r.end_s[:, cols].astype(BF16)
        lead_grad = r.lead_w[:, cols] * r.grad[:, cols].astype(F32)
        gather("reads", k, head_sum(lead_grad * mm(r.proj[:, state_dim:], inc), hot))
        gather("gc", k, mm_nt(r.lg[:, cols], inc))

    def inner_tail(k):
        cols = cols_of(k)
        hot = r.hot[:heads, cols]
        gather("cols", k, head_sum(r.u[:, cols].astype(F32) * r.gu[:, cols], hot))
        products = r.values[:, cols].astype(F32) * r.grad[:, cols].astype(F32)
        products = jnp.sum(products, axis=0, keepdims=True)
        gather("skips", k, head_sum(jnp.broadcast_to(products, (8, span)), hot))

    def backward_tail(k):
        copy(4, "g", k).wait_recv()
        cols = cols_of(k)
        hot = r.hot[:heads, cols]
        outgoing = r.end_g[:, cols]
        out = outgoing.astype(BF16)
        values = r.values[:, cols].astype(F32)
        gather("gb", k, mm_nt(r.tsv[:, cols], out))
        back = r.tail_w[:, cols] * mm(r.proj[:, :state_dim], out)
        gather("backs", k, head_sum(values * back, hot))
        gu = r.gu[:, cols] + back
        gather("gsteps", k, head_sum(values * gu, hot))
        cross = jnp.sum(r.end_s[:, cols] * outgoing, axis=0, keepdims=True)
        gather("cross", k, head_sum(jnp.broadcast_to(cross, (8, span)), hot))
        gain = mm(stacked(jnp.broadcast_to(r.gain[...], (8, heads))), r.hot3[:, cols])[0:1]
        gvalues_ref[:, cols] = (
            r.step_w[:, cols] * gu + gain * r.grad[:, cols].astype(F32)
        ).astype(BF16)

    plan = reduce_plan(depth, devices, heads)
    share, lanes, group = packing(depth, devices, heads)

    def places(order):
        return [
            sum(((shard >> order[i]) & 1) * (devices >> (i + 1)) for i in range(levels))
            for shard in range(devices)
        ]

    def offset(order, count):
        result = 0
        for i in range(count):
            result = result + bits[order[i]] * (devices >> (i + 1))
        return result

    def part(q, i, which):
        size, order = plan[q][2], plan[q][3]
        start = (offset(order, i) + which * (devices >> (i + 1))) * size
        return pl.ds(pl.multiple_of(start, 8), (devices >> (i + 1)) * size)

    def reduce_copy(q, i):
        k = plan[q][3][i]
        return remote(
            getattr(r, f"sum{q}").at[part(q, i, 1 - bits[k])], getattr(r, f"rget{q}_{i}"),
            r.rsem.at[0, i, q], r.rsem.at[1, i, q], partners[k],
        )

    def reduce_step(q, i):
        k = plan[q][3][i]
        reduce_copy(q, i).wait_recv()
        sums = getattr(r, f"sum{q}")
        mine = part(q, i, bits[k])
        sums[mine] = sums[mine] + getattr(r, f"rget{q}_{i}")[...]
        if i + 1 < levels:
            reduce_copy(q, i + 1).start()

    def send_piece(q):
        plane, first, size, order = plan[q]
        grad = r.gproj[:, plane * state_dim : (plane + 1) * state_dim]
        sums = getattr(r, f"sum{q}")
        where = places(order)
        product = mm(r.layer_t[devices * first : devices * (first + size)], grad)
        for shard in range(devices):
            sums[where[shard] * size : (where[shard] + 1) * size] = (
                product[shard * size : (shard + 1) * size])
        reduce_copy(q, 0).start()

    def finish_c():
        grad_c = r.gc[...] + mm_tn(r.gscores[...].astype(BF16), r.proj[:, :state_dim])
        grad_c = grad_c.astype(BF16)
        r.gproj[:, state_dim : 2 * state_dim] = grad_c

    def finish_b():
        grad_b = r.gb[...] + mm(r.gscores[...].astype(BF16), r.proj[:, state_dim:])
        grad_b = grad_b.astype(BF16)
        r.gproj[:, :state_dim] = grad_b

    def before_dt():
        upper = triangle(tokens, lambda a, b: a <= b)
        inner = r.rows[:, 0, :].T + r.reads[...] - r.cols[...]
        r.pre[...] = exact_mm(upper, inner)
        r.sigmoid[...] = 1.0 / (1.0 + jnp.exp(-r.raw[...]))

    def finish_dt():
        step = r.step[...]
        rate = jnp.exp(r.rate[...])
        total = r.run[tokens - 1 :, :]
        lower = triangle(tokens, lambda a, b: a > b)
        grad_decay = (
            r.pre[...] + exact_mm(lower, step * r.backs[...]) + jnp.exp(total) * r.cross[0:1]
        )
        grad_raw = (r.gsteps[...] - rate * grad_decay) * r.sigmoid[...]
        r.gproj[:, 2 * state_dim :] = grad_raw.astype(BF16)
        small = jnp.concatenate([
            jnp.sum(grad_raw, axis=0, keepdims=True),
            -rate * jnp.sum(grad_decay * step, axis=0, keepdims=True),
            r.skips[0:1],
            jnp.zeros((5, heads), F32),
        ], axis=0)
        r.small[...] = jnp.concatenate([small, jnp.zeros((8, TILE - heads), F32)], axis=1)

    def send_dt():
        narrow = r.gproj[:, 2 * state_dim :]
        product = mm(r.layer_t[...], jnp.concatenate(
            [narrow.astype(F32), jnp.zeros((tokens, TILE - heads), F32)], axis=1).astype(BF16))
        small = r.small[...]

        def shard_rows(shard, begin, count):
            found, first = [], 0
            for size in pieces_of(share):
                low, high = max(begin, first), min(begin + count, first + size)
                if low < high:
                    base = devices * first + shard * size - first
                    found.append(product[base + low : base + high])
                first += size
            return found[0] if len(found) == 1 else jnp.concatenate(found, axis=0)

        q = len(plan) - 1
        unit = group + 8
        sums = getattr(r, f"sum{q}")
        where = places(plan[q][3])
        for shard in range(devices):
            start = where[shard] * unit
            packed = jnp.zeros((group, TILE), F32)
            for j in range(lanes):
                count = min(share - j * group, group)
                if count <= 0:
                    continue
                piece = shard_rows(shard, j * group, count)
                if j > 0:
                    piece = pltpu.roll(piece, j * heads, 1)
                if count < group:
                    piece = jnp.concatenate(
                        [piece, jnp.zeros((group - count, TILE), F32)], axis=0)
                packed = packed + piece
            sums[start : start + group] = packed
            sums[start + group : start + unit] = small
        reduce_copy(q, 0).start()

    def layer_tail(k):
        cols = slice(k * depth // TAILS, (k + 1) * depth // TAILS)
        glayer_ref[:, cols] = (
            mm_nt(r.gproj[:, : 2 * state_dim], r.wbc[cols])
            + mm(r.gproj[:, 2 * state_dim :], r.wdt[:, cols])
        ).astype(BF16)

    def prepare():
        run = r.run[...]
        run_rows = run.T
        for head in range(heads):
            r.run_rows[head] = run_rows[head : head + 1]
        r.parts[...] = stacked(run)
        r.scores[...] = mm_nt(r.proj[:, :state_dim], r.proj[:, state_dim:])
        r.gscores[...] = jnp.zeros_like(r.gscores)

    def turn():
        turned = r.layer[...].T
        first = 0
        for size in pieces_of(share):
            for shard in range(devices):
                start, target = shard * share + first, devices * first + shard * size
                r.layer_t[target : target + size] = turned[start : start + size]
            first += size

    def body(pair, _):
        inner_pair(pair, heads, r.u, r.grad, r.scores, r.parts, r.run_rows,
                   r.gu, r.rows, r.gscores, head_size)
        return 0

    n = CHUNKS
    wire, flight, near, hop_wire, hop = 7.05 / n, 3.0, 1.1, 7.2 / (2 * n), 2.9 + 3.6 / n
    blocks = n // BLOCK
    pool, link = [], {"y": 0.0, "s": 0.0, "g": 0.0, "z": 0.0, "m": 0.0}
    clock, serial = [3.2], [0]
    left = {"s": n, "g": n}

    def add(ready, rank, cost, work, args=(), after=None):
        serial[0] += 1
        pool.append((ready, rank, serial[0], cost, work, args, after))

    def through(name, now, time):
        link[name] = max(link[name], now) + time
        return link[name]

    def after_make(kind, block):
        def after(now):
            for k in range(block * BLOCK, (block + 1) * BLOCK):
                add(now + near, 0, 0.02, pair_up, (kind, k), after_pair(kind, k))
        return after

    def after_pair(kind, k):
        def after(now):
            add(through("y", now, wire) + flight, 0, 0.02, row_up, (kind, k),
                lambda now: add(now, 0, 0.01, chain_slot, (kind, k, 0), after_chain(kind, k, 0)))
        return after

    def after_chain(kind, k, place):
        def after(now):
            if place + 1 < zrows:
                add(through(kind, now, hop_wire) + hop, 0, 0.01, chain_slot,
                    (kind, k, place + 1), after_chain(kind, k, place + 1))
            else:
                add(now, 0, 0.02, row_down, (kind, k), after_down(kind, k))
        return after

    def after_down(kind, k):
        def after(now):
            add(through("y", now, wire) + flight, 0, 0.02, chip_down, (kind, k),
                lambda now: add(now + near, 1, 4.1 / n if kind == "s" else 5.0 / n,
                                forward_tail if kind == "s" else backward_tail, (k,),
                                after_tail(kind)))
        return after

    def after_tail(kind):
        def after(now):
            left[kind] -= 1
            if left[kind] == 0:
                add(now, 1, 0.22, finish_c if kind == "s" else finish_b, (), after_finish(kind))
        return after

    def after_dt(now):
        add(now, 1, 0.9, send_dt, (), after_send(len(plan) - 1))
        for k in range(TAILS):
            soft.append((1.5 / TAILS, functools.partial(layer_tail, k)))

    def after_finish(kind):
        def after(now):
            for q, (plane, first, size, order) in enumerate(plan):
                if plane == (1 if kind == "s" else 0):
                    add(now, 1, size * 0.007, send_piece, (q,), after_send(q))
            if kind == "g":
                add(now + 0.01, 1, 0.31, finish_dt, (), after_dt)
        return after

    def after_send(q):
        arrive = near + (0.5 if plan[q][0] == 2 else 0.0)
        return lambda now: add(now + arrive, 0, 0.03, reduce_step, (q, 0), after_reduce(q, 0))

    def after_reduce(q, i):
        def after(now):
            if i + 1 == levels:
                return
            level = plan[q][3][i + 1]
            pace = plan[q][2] * 0.045 / (1 << i)
            if level == 1:
                arrive = through("y", now, pace) + 2.8
            elif level == 2:
                arrive = through("z", now, pace) + 2.8
            else:
                through("z", now, pace)
                arrive = through("m", now, 2 * pace) + 3.5
            if i + 2 == levels:
                arrive += 1000.0
            add(arrive, 0, 0.02, reduce_step, (q, i + 1), after_reduce(q, i + 1))
        return after

    for block in range(blocks):
        add(0.0, 1, 2.25 / blocks, make_states, ("s", block), after_make("s", block))
    for block in range(blocks):
        add(0.1, 1, 1.9 / blocks, make_states, ("g", block), after_make("g", block))
    add(4.0, 0, 0.25, tot_done, (0,))
    add(7.0, 0, 0.25, tot_done, (1,))

    pairs = width // TILE
    soft = [(0.25, prepare)] + [(0.46, None)] * pairs + [(0.4, turn)]
    soft += [(1.7 / n, functools.partial(inner_tail, k)) for k in range(n)] + [(0.4, before_dt)]
    pending = [0, 0]

    def flush_pairs():
        if pending[1]:
            lax.fori_loop(pending[0], pending[0] + pending[1], body, 0)
            pending[0], pending[1] = pending[0] + pending[1], 0

    def soften():
        cost, work = soft.pop(0)
        clock[0] += cost
        if work is None:
            pending[1] += 1
        else:
            flush_pairs()
            work()

    while pool:
        ready = [item for item in pool if item[0] <= clock[0] + 1e-6]
        if not ready:
            following = min(item[0] for item in pool)
            usable = soft and (soft[0][1] is not before_dt or left["s"] == 0)
            if usable and clock[0] + soft[0][0] <= following + 0.25:
                soften()
            else:
                clock[0] = following
            continue
        item = min(ready, key=lambda entry: (entry[1], entry[0], entry[2]))
        pool.remove(item)
        cost, work, args, after = item[3:]
        if work in (finish_c, backward_tail):
            while soft and soft[0][1] is not before_dt:
                soften()
        if work is finish_dt or item[0] > 1000.0:
            while soft:
                soften()
        flush_pairs()
        work(*args)
        clock[0] += cost
        if after:
            after(clock[0])

    for q, (plane, first, size, order) in enumerate(plan):
        unit = size
        start = pl.multiple_of(offset(order, levels) * unit, 8)
        result = getattr(r, f"sum{q}")[pl.ds(start, unit)]
        if plane < 2:
            gbc_ref[first : first + size, plane * TILE : (plane + 1) * TILE] = result
        else:
            last_ref[...] = result
    for k in range(2):
        tot_copy(k).wait_send()
    for kind in kinds:
        for k in range(n):
            for stage in (0, 1, 3, 4):
                copy(stage, kind, k).wait_send()
        if zrows > 1:
            sends = row < zrows - 1 if kind == "s" else row > 0

            @pl.when(sends)
            def _(kind=kind):
                for k in range(n):
                    copy(2, kind, k).wait_send()
    for q in range(len(plan)):
        for i in range(levels):
            reduce_copy(q, i).wait_send()


def finish_kernel(heads, group, lanes, gvalues_in, glayer_in, gbc_in, last_in,
                  gvalues_ref, glayer_ref, gbc_ref, gdt_ref, gbias_ref, grate_ref, gskip_ref, sems):
    copies = [
        pltpu.make_async_copy(source, target, sems.at[i])
        for i, (source, target) in enumerate((
            (gvalues_in, gvalues_ref), (glayer_in, glayer_ref), (gbc_in, gbc_ref),
        ))
    ]
    for copy in copies:
        copy.start()
    last = last_in[...]
    share = gdt_ref.shape[1]
    pieces = []
    for j in range(lanes):
        count = min(share - j * group, group)
        if count > 0:
            pieces.append(last[:count, j * heads : (j + 1) * heads])
    gdt_ref[...] = jnp.concatenate(pieces, axis=0).T
    gbias_ref[...] = last[group : group + 1, :heads]
    grate_ref[...] = last[group + 1 : group + 2, :heads]
    gskip_ref[...] = last[group + 2 : group + 3, :heads]
    for copy in copies:
        copy.wait()


def local(layer_in, ssm_in, weight_bc, weight_dt, bias_dt, log_rate, skip_gain, grad_out):
    tokens, depth = layer_in.shape
    heads = log_rate.shape[0]
    width = ssm_in.shape[1]
    state_dim = weight_bc.shape[1] // 2
    devices = lax.axis_size("seq")
    share, lanes, group = packing(depth, devices, heads)
    scratch = scratch_list(tokens, depth, width, heads, state_dim, devices)
    shape = jax.ShapeDtypeStruct
    gvalues, glayer, gbc, last = pl.pallas_call(
        functools.partial(mega_kernel, devices, list(scratch)),
        out_shape=[
            pltpu.VMEM((tokens, width), BF16),
            pltpu.VMEM((tokens, depth), BF16),
            pltpu.VMEM((share, 2 * state_dim), F32),
            pltpu.VMEM((group + 8, TILE), F32),
        ],
        in_specs=[ANY] * 8,
        out_specs=[VMEM, VMEM, VMEM, VMEM],
        scratch_shapes=list(scratch.values()),
        compiler_params=pltpu.CompilerParams(
            collective_id=0, has_side_effects=True, vmem_limit_bytes=VMEM_LIMIT
        ),
        name="mixer",
    )(layer_in, ssm_in, weight_bc, weight_dt.T, bias_dt[None, :], log_rate[None, :],
      skip_gain[None, :], grad_out)
    outs = pl.pallas_call(
        functools.partial(finish_kernel, heads, group, lanes),
        out_shape=[
            shape((tokens, width), BF16),
            shape((tokens, depth), BF16),
            shape((share, 2 * state_dim), F32),
            shape((heads, share), F32),
            shape((1, heads), F32),
            shape((1, heads), F32),
            shape((1, heads), F32),
        ],
        in_specs=[VMEM] * 4,
        out_specs=[ANY] * 3 + [VMEM] * 4,
        scratch_shapes=[pltpu.SemaphoreType.DMA((3,))],
        compiler_params=pltpu.CompilerParams(vmem_limit_bytes=8 * 1024 * 1024),
        name="finish",
    )(gvalues, glayer, gbc, last)
    return tuple(outs[:3]) + (outs[3].T,) + tuple(out[0] for out in outs[4:])


def solution(mesh):
    rows = P(("groups", "seq"), None)
    in_specs = (rows, rows, P(), P(), P(), P(), P(), rows)
    out_specs = (rows, rows, rows, rows, P("groups"), P("groups"), P("groups"))
    return jax.shard_map(local, mesh=mesh, in_specs=in_specs, out_specs=out_specs, check_vma=False)
```

```python
import functools
import jax
import jax.numpy as jnp
from jax import lax
from jax.experimental import pallas as pl
from jax.experimental.pallas import tpu as pltpu
from jax.sharding import PartitionSpec as P

F32 = jnp.float32
BF16 = jnp.bfloat16
TILE = 128
CHUNKS = 10
BLOCK = 2
TAILS = 4
LOADS = 4
REDUCE_C, REDUCE_B, REDUCE_DT = "zzyy", "yyyz", "z"
VMEM_LIMIT = 52 * 1024 * 1024
VMEM = pl.BlockSpec(memory_space=pltpu.VMEM)
ANY = pl.BlockSpec(memory_space=pl.ANY)


def mm(left, right):
    return lax.dot_general(left, right, (((1,), (0,)), ((), ())), preferred_element_type=F32)


def mm_nt(left, right):
    return lax.dot_general(left, right, (((1,), (1,)), ((), ())), preferred_element_type=F32)


def mm_tn(left, right):
    return lax.dot_general(left, right, (((0,), (0,)), ((), ())), preferred_element_type=F32)


def three_way(x):
    high = x.astype(BF16)
    rest = x - high.astype(F32)
    middle = rest.astype(BF16)
    return high, middle, (rest - middle.astype(F32)).astype(BF16)


def one_hot(heads, width, columns, first=0):
    row = lax.broadcasted_iota(jnp.int32, (heads, columns), 0)
    col = lax.broadcasted_iota(jnp.int32, (heads, columns), 1) + first
    inside = (col >= row * width) & (col < (row + 1) * width)
    return jnp.where(inside, 1.0, 0.0).astype(BF16)


def one_hot_stacked(heads, width, columns, first=0):
    row = lax.rem(lax.broadcasted_iota(jnp.int32, (TILE, columns), 0), heads)
    real = lax.broadcasted_iota(jnp.int32, (TILE, columns), 0) < 3 * heads
    col = lax.broadcasted_iota(jnp.int32, (TILE, columns), 1) + first
    inside = (col >= row * width) & (col < (row + 1) * width) & real
    return jnp.where(inside, 1.0, 0.0).astype(BF16)


def stacked(x):
    rows, heads = x.shape
    zero = jnp.zeros((rows, TILE - heads), F32)
    result = None
    for i, piece in enumerate(three_way(x)):
        piece = jnp.concatenate([piece.astype(F32), zero], axis=1)
        piece = piece if i == 0 else pltpu.roll(piece, i * heads, 1)
        result = piece if i == 0 else result + piece
    return result.astype(BF16)


def head_sum(x, hot):
    high = x.astype(BF16)
    low = (x - high.astype(F32)).astype(BF16)
    return mm_nt(high, hot) + mm_nt(low, hot)


def exact_mm(mask, x):
    parts = three_way(x)
    return mm(mask, parts[0]) + mm(mask, parts[1]) + mm(mask, parts[2])


def triangle(size, compare):
    row = lax.broadcasted_iota(jnp.int32, (size, size), 0)
    col = lax.broadcasted_iota(jnp.int32, (size, size), 1)
    return jnp.where(compare(row, col), 1.0, 0.0).astype(BF16)


def inner_pair(pair, heads, u_ref, grad_ref, scores_ref, parts_ref, run_rows_ref,
               gu_ref, rows_ref, gscores_ref, head_size):
    tokens = u_ref.shape[0]
    blocks = tokens // TILE
    per = TILE // head_size
    cols = pl.ds(pl.multiple_of(pair * TILE, TILE), TILE)
    lane = lax.broadcasted_iota(jnp.int32, (TILE, TILE), 1)
    causal = lax.broadcasted_iota(jnp.int32, (TILE, TILE), 0) <= lane
    wide = one_hot_stacked(heads, TILE, per * TILE, pair * (per * TILE))
    run_cols = mm(parts_ref[...], wide)
    grads = [grad_ref[t * TILE : (t + 1) * TILE, cols] for t in range(blocks)]
    gus = [jnp.zeros((TILE, TILE), F32) for _ in range(blocks)]
    for sub in range(per):
        head = pair * per + sub
        keep = (lane >= sub * head_size) & (lane < (sub + 1) * head_size)
        rows = [jnp.zeros((1, TILE), F32) for _ in range(blocks)]
        for s in range(blocks):
            srange = slice(s * TILE, (s + 1) * TILE)
            run_col = run_cols[srange, sub * TILE : (sub + 1) * TILE]
            u_head = jnp.where(keep, u_ref[srange, cols], jnp.zeros((), BF16))
            gu = jnp.zeros((TILE, TILE), F32)
            for t in range(s, blocks):
                trange = slice(t * TILE, (t + 1) * TILE)
                gap = run_rows_ref[head, :, trange] - run_col
                if s == t:
                    gap = jnp.where(causal, gap, -jnp.inf)
                factor = jnp.exp(gap)
                mixing = (factor * scores_ref[srange, trange]).astype(BF16)
                weight = mm_nt(u_head, grads[t])
                gscores_ref[srange, trange] += factor * weight
                rows[t] += jnp.sum(mixing.astype(F32) * weight, axis=0, keepdims=True)
                gu += mm(mixing, grads[t])
            gus[s] = jnp.where(keep, gu, gus[s])
        for t in range(blocks):
            rows_ref[head, :, t * TILE : (t + 1) * TILE] = rows[t]
    for s in range(blocks):
        gu_ref[s * TILE : (s + 1) * TILE, cols] = gus[s]


def packing(depth, devices, heads):
    share = depth // devices
    lanes = TILE // heads
    group = -(-share // (8 * lanes)) * 8
    return share, lanes, group


def pieces_of(share):
    units = share // 16
    if share % 16 or units < 4:
        return [share]
    return [16 * ((units + 3 - i) // 4) for i in range(4)]


def reduce_plan(depth, devices, heads):
    share, lanes, group = packing(depth, devices, heads)
    levels = devices.bit_length() - 1
    y_first = list(range(levels))
    z_first = [0] + list(range(2, levels)) + [1]
    plan, first = [], 0
    cuts = pieces_of(share)
    for plane, names in ((1, REDUCE_C), (0, REDUCE_B)):
        first = 0
        for piece, size in enumerate(cuts):
            plan.append((plane, first, size, y_first if names[piece] == "y" else z_first))
            first += size
    plan.append((2, 0, group + 8, y_first if REDUCE_DT == "y" else z_first))
    return plan


def scratch_list(tokens, depth, width, heads, state_dim, devices):
    levels = devices.bit_length() - 1
    half, quarter = state_dim // 2, state_dim // 4
    plan = reduce_plan(depth, devices, heads)
    names = {}

    def add(name, shape, dtype=F32):
        names[name] = pltpu.VMEM(shape, dtype)

    add("layer", (tokens, depth), BF16)
    add("values", (tokens, width), BF16)
    add("grad", (tokens, width), BF16)
    add("wbc", (depth, 2 * state_dim), BF16)
    add("wdt", (heads, depth), BF16)
    add("layer_t", (depth, tokens), BF16)
    add("proj", (tokens, 2 * state_dim), BF16)
    add("proj_t", (2 * state_dim, tokens), BF16)
    add("hot", (TILE, width), BF16)
    for name in ("parts", "step3", "tail3", "lead3"):
        add(name, (tokens, TILE), BF16)
    add("hot3", (TILE, width), BF16)
    for name in ("bias", "rate", "gain"):
        add(name, (1, heads))
    add("pre", (tokens, heads))
    add("sigmoid", (tokens, heads))
    for name in ("raw", "step", "run"):
        add(name, (tokens, heads))
    add("run_rows", (heads, 1, tokens))
    add("rows", (heads, 1, tokens))
    add("scores", (tokens, tokens))
    add("gscores", (tokens, tokens))
    for name in ("step_w", "lead_w", "tail_w", "gu"):
        add(name, (tokens, width))
    for name in ("u", "tsv", "lg"):
        add(name, (tokens, width), BF16)
    for name in ("reads", "cols", "backs", "gsteps"):
        add(name, (tokens, heads))
    add("cross", (8, heads))
    add("skips", (8, heads))
    add("small", (8, TILE))
    add("gc", (tokens, state_dim))
    add("gb", (tokens, state_dim))
    add("gproj", (tokens, 2 * state_dim + heads), BF16)
    for kind in ("s", "g"):
        add("st_" + kind, (state_dim, width))
        add("get0_" + kind, (half, width))
        add("agg1_" + kind, (half, width))
        add("get1_" + kind, (quarter, width))
        add("agg2_" + kind, (quarter, width))
        add("zin_" + kind, (quarter, width))
        add("zout_" + kind, (quarter, width))
        add("send1_" + kind, (quarter, width))
        add("chip_" + kind, (half, width))
        add("send0_" + kind, (half, width))
        add("end_" + kind, (state_dim, width))
    add("tots", (2, 8, TILE))
    add("tot_gets", (2, 8, TILE))
    add("decays", (5, 8, width))
    for q, (plane, first, size, order) in enumerate(plan):
        add(f"sum{q}", (devices * size, TILE))
        for i in range(levels):
            add(f"rget{q}_{i}", ((devices >> (i + 1)) * size, TILE))
    add_sem = lambda name, shape: names.__setitem__(name, pltpu.SemaphoreType.DMA(shape))
    add_sem("load", (6,))
    add_sem("early", (2, LOADS))
    add_sem("comm", (2, 5, 2, CHUNKS))
    add_sem("tot_sems", (2, 2))
    add_sem("rsem", (2, levels, len(plan)))
    return names


class Box:
    pass


def mega_kernel(devices, names, layer_hbm, values_hbm, wbc_hbm, wdt_hbm, bias_hbm, rate_hbm,
                gain_hbm, grad_hbm, gvalues_ref, glayer_ref, gbc_ref, last_ref, *refs):
    r = Box()
    for name, ref in zip(names, refs):
        setattr(r, name, ref)
    tokens, depth = r.layer.shape
    width = r.values.shape[1]
    heads = r.bias.shape[1]
    head_size = width // heads
    state_dim = r.st_s.shape[0]
    half, quarter = state_dim // 2, state_dim // 4
    levels = devices.bit_length() - 1
    zrows = devices // 4
    span = width // CHUNKS
    me = lax.axis_index("seq")
    bits = [lax.rem(me // (1 << k), 2) for k in range(levels)]
    partners = [me + (1 - 2 * bits[k]) * (1 << k) for k in range(levels)]
    row = me // 4
    up_row = lax.rem(me + 4, devices)
    down_row = lax.rem(me + devices - 4, devices)
    mesh_id = pl.DeviceIdType.MESH

    pieces = [slice(i * depth // LOADS, (i + 1) * depth // LOADS) for i in range(LOADS)]
    early = [
        [
            pltpu.make_async_copy(source, target, r.early.at[j, i])
            for j, (source, target) in enumerate((
                (layer_hbm.at[:, piece], r.layer.at[:, piece]),
                (wbc_hbm.at[piece], r.wbc.at[piece]),
            ))
        ]
        for i, piece in enumerate(pieces)
    ]
    loads = [
        pltpu.make_async_copy(source, target, r.load.at[i])
        for i, (source, target) in enumerate((
            (wdt_hbm, r.wdt), (bias_hbm, r.bias), (rate_hbm, r.rate), (gain_hbm, r.gain),
            (values_hbm, r.values), (grad_hbm, r.grad),
        ))
    ]
    for i in range(4):
        loads[i].start()
    for group in early:
        for load in group:
            load.start()
    for i in (4, 5):
        loads[i].start()

    barrier = pltpu.get_barrier_semaphore()
    for k in range(levels):
        pl.semaphore_signal(barrier, inc=1, device_id={"seq": partners[k]}, device_id_type=mesh_id)
    if zrows > 1:
        @pl.when(row < zrows - 1)
        def _():
            pl.semaphore_signal(barrier, inc=1, device_id={"seq": up_row}, device_id_type=mesh_id)

        @pl.when(row > 0)
        def _():
            pl.semaphore_signal(barrier, inc=1, device_id={"seq": down_row}, device_id_type=mesh_id)

    r.hot[...] = one_hot(TILE, head_size, width)
    r.hot3[...] = one_hot_stacked(heads, head_size, width)
    for i in range(4):
        loads[i].wait()
    proj, raw = None, None
    for piece, group in zip(pieces, early):
        for load in group:
            load.wait()
        layer = r.layer[:, piece]
        add_raw = mm_nt(layer, r.wdt[:, piece])
        add_proj = mm(layer, r.wbc[piece])
        proj = add_proj if proj is None else proj + add_proj
        raw = add_raw if raw is None else raw + add_raw
    raw = raw + r.bias[...]
    r.raw[...] = raw
    proj = proj.astype(BF16)
    r.proj[...] = proj
    r.proj_t[...] = proj.T
    step = jnp.maximum(raw, 0.0) + jnp.log1p(jnp.exp(-jnp.abs(raw)))
    r.step[...] = step
    decay = -jnp.exp(r.rate[...]) * step
    run = exact_mm(triangle(tokens, lambda a, b: a >= b), decay)
    r.run[...] = run
    total = run[tokens - 1 :, :]
    r.step3[...] = stacked(step)
    r.tail3[...] = stacked(jnp.exp(total - run))
    r.tots[0] = jnp.zeros((8, TILE), F32)
    r.tots[0, :, :heads] = jnp.broadcast_to(total, (8, heads))
    if zrows > 1:
        count = levels + jnp.where(row < zrows - 1, 1, 0) + jnp.where(row > 0, 1, 0)
    else:
        count = levels
    pl.semaphore_wait(barrier, count)

    def remote(source, target, send, receive, device):
        return pltpu.make_async_remote_copy(
            src_ref=source, dst_ref=target, send_sem=send, recv_sem=receive,
            device_id={"seq": device}, device_id_type=mesh_id,
        )

    def tot_copy(k):
        return remote(r.tots.at[k], r.tot_gets.at[k], r.tot_sems.at[0, k], r.tot_sems.at[1, k],
                      partners[k])

    tot_copy(0).start()

    kinds = ("s", "g")

    def cols_of(k):
        return slice(k * span, (k + 1) * span)

    def at(name, kind):
        return getattr(r, name + "_" + kind)

    def rows_at(which, size):
        return pl.ds(pl.multiple_of(which * size, 8), size)

    def copy(stage, kind, k):
        cols = cols_of(k)
        if stage == 0:
            source = at("st", kind).at[rows_at(1 - bits[0], half), cols]
            target, device = at("get0", kind).at[:, cols], partners[0]
        elif stage == 1:
            source = at("agg1", kind).at[rows_at(1 - bits[1], quarter), cols]
            target, device = at("get1", kind).at[:, cols], partners[1]
        elif stage == 2:
            source, target = at("zout", kind).at[:, cols], at("zin", kind).at[:, cols]
            device = up_row if kind == "s" else down_row
        elif stage == 3:
            source = at("send1", kind).at[:, cols]
            target, device = at("chip", kind).at[rows_at(bits[1], quarter), cols], partners[1]
        else:
            source = at("send0", kind).at[:, cols]
            target, device = at("end", kind).at[rows_at(bits[0], half), cols], partners[0]
        i = kinds.index(kind)
        return remote(source, target, r.comm.at[0, stage, i, k], r.comm.at[1, stage, i, k], device)

    def tot_done(k):
        tot_copy(k).wait_recv()
        mine, other = r.tots[k], r.tot_gets[k]
        both = jnp.concatenate([mine, other], axis=0)
        stacked = jnp.concatenate(list(three_way(both)), axis=0)
        wide = mm(stacked, r.hot[...])
        wide = jnp.exp(wide[0:16] + wide[16:32] + wide[32:48])
        r.decays[2 * k] = wide[0:8]
        r.decays[2 * k + 1] = wide[8:16]
        if k == 0:
            r.tots[1] = mine + other
            tot_copy(1).start()
        else:
            r.decays[4] = wide[0:8] * wide[8:16]

    first0, first1 = bits[0] == 0, bits[1] == 0

    def make_states(kind, block):
        if block == 0:
            loads[4 if kind == "s" else 5].wait()
        cols = slice(block * BLOCK * span, (block + 1) * BLOCK * span)
        hot = r.hot3[:, cols]
        if kind == "s":
            step_w = mm(r.step3[...], hot)
            r.step_w[:, cols] = step_w
            tail_w = mm(r.tail3[...], hot)
            r.tail_w[:, cols] = tail_w
            u = step_w * r.values[:, cols].astype(F32)
            r.u[:, cols] = u.astype(BF16)
            tsv = (tail_w * u).astype(BF16)
            r.tsv[:, cols] = tsv
            r.st_s[:, cols] = mm(r.proj_t[:state_dim], tsv)
        else:
            if block == 0:
                r.lead3[...] = stacked(jnp.exp(r.run[...]))
            lead_w = mm(r.lead3[...], hot)
            r.lead_w[:, cols] = lead_w
            lg = (lead_w * r.grad[:, cols].astype(F32)).astype(BF16)
            r.lg[:, cols] = lg
            r.st_g[:, cols] = mm(r.proj_t[state_dim:], lg)
        for k in range(block * BLOCK, (block + 1) * BLOCK):
            copy(0, kind, k).start()

    def merge(kind, first, mine, got, e_mine, e_other):
        if kind == "s":
            return jnp.where(first, e_other * mine + got, mine + e_mine * got)
        return jnp.where(first, mine + e_mine * got, e_other * mine + got)

    def split(kind, first, parent, mine, got, e_mine, e_other):
        far, near = e_other * parent + got, e_mine * parent + mine
        if kind == "s":
            return jnp.where(first, parent, far), jnp.where(first, near, parent)
        return jnp.where(first, far, parent), jnp.where(first, parent, near)

    def pair_up(kind, k):
        copy(0, kind, k).wait_recv()
        cols = cols_of(k)
        mine = at("st", kind)[rows_at(bits[0], half), cols]
        got = at("get0", kind)[:, cols]
        at("agg1", kind)[:, cols] = merge(
            kind, first0, mine, got, r.decays[0, 0:1, cols], r.decays[1, 0:1, cols])
        copy(1, kind, k).start()

    def row_up(kind, k):
        copy(1, kind, k).wait_recv()
        cols = cols_of(k)
        mine = at("agg1", kind)[rows_at(bits[1], quarter), cols]
        got = at("get1", kind)[:, cols]
        at("agg2", kind)[:, cols] = merge(
            kind, first1, mine, got, r.decays[2, 0:1, cols], r.decays[3, 0:1, cols])

    def chain(kind, k, place):
        cols = cols_of(k)
        if place > 0:
            copy(2, kind, k).wait_recv()
            parent = at("zin", kind)[:, cols]
        else:
            parent = jnp.zeros((quarter, span), F32)
        if place < zrows - 1:
            passed = at("agg2", kind)[:, cols]
            if place > 0:
                passed = r.decays[4, 0:1, cols] * parent + passed
            at("zout", kind)[:, cols] = passed
            copy(2, kind, k).start()
        if place == 0:
            at("zin", kind)[:, cols] = parent

    def row_down(kind, k):
        cols = cols_of(k)
        parent = at("zin", kind)[:, cols]
        mine = at("agg1", kind)[rows_at(bits[1], quarter), cols]
        got = at("get1", kind)[:, cols]
        kept, sent = split(kind, first1, parent, mine, got,
                           r.decays[2, 0:1, cols], r.decays[3, 0:1, cols])
        at("send1", kind)[:, cols] = sent
        copy(3, kind, k).start()
        at("chip", kind)[rows_at(bits[1], quarter), cols] = kept

    def chain_slot(kind, k, place):
        where = place if kind == "s" else zrows - 1 - place
        if zrows == 1:
            chain(kind, k, place)
        else:
            pl.when(row == where)(lambda: chain(kind, k, place))

    def chip_down(kind, k):
        copy(3, kind, k).wait_recv()
        cols = cols_of(k)
        parent = at("chip", kind)[:, cols]
        mine = at("st", kind)[rows_at(bits[0], half), cols]
        got = at("get0", kind)[:, cols]
        kept, sent = split(kind, first0, parent, mine, got,
                           r.decays[0, 0:1, cols], r.decays[1, 0:1, cols])
        at("send0", kind)[:, cols] = sent
        copy(4, kind, k).start()
        at("end", kind)[rows_at(bits[0], half), cols] = kept

    def gather(name, k, x):
        ref = getattr(r, name)
        ref[...] = x if k == 0 else ref[...] + x

    def forward_tail(k):
        copy(4, "s", k).wait_recv()
        cols = cols_of(k)
        hot = r.hot[:heads, cols]
        inc = r.end_s[:, cols].astype(BF16)
        lead_grad = r.lead_w[:, cols] * r.grad[:, cols].astype(F32)
        gather("reads", k, head_sum(lead_grad * mm(r.proj[:, state_dim:], inc), hot))
        gather("gc", k, mm_nt(r.lg[:, cols], inc))

    def inner_tail(k):
        cols = cols_of(k)
        hot = r.hot[:heads, cols]
        gather("cols", k, head_sum(r.u[:, cols].astype(F32) * r.gu[:, cols], hot))
        products = r.values[:, cols].astype(F32) * r.grad[:, cols].astype(F32)
        products = jnp.sum(products, axis=0, keepdims=True)
        gather("skips", k, head_sum(jnp.broadcast_to(products, (8, span)), hot))

    def backward_tail(k):
        copy(4, "g", k).wait_recv()
        cols = cols_of(k)
        hot = r.hot[:heads, cols]
        outgoing = r.end_g[:, cols]
        out = outgoing.astype(BF16)
        values = r.values[:, cols].astype(F32)
        gather("gb", k, mm_nt(r.tsv[:, cols], out))
        back = r.tail_w[:, cols] * mm(r.proj[:, :state_dim], out)
        gather("backs", k, head_sum(values * back, hot))
        gu = r.gu[:, cols] + back
        gather("gsteps", k, head_sum(values * gu, hot))
        cross = jnp.sum(r.end_s[:, cols] * outgoing, axis=0, keepdims=True)
        gather("cross", k, head_sum(jnp.broadcast_to(cross, (8, span)), hot))
        gain = mm(stacked(jnp.broadcast_to(r.gain[...], (8, heads))), r.hot3[:, cols])[0:1]
        gvalues_ref[:, cols] = (
            r.step_w[:, cols] * gu + gain * r.grad[:, cols].astype(F32)
        ).astype(BF16)

    plan = reduce_plan(depth, devices, heads)
    share, lanes, group = packing(depth, devices, heads)

    def places(order):
        return [
            sum(((shard >> order[i]) & 1) * (devices >> (i + 1)) for i in range(levels))
            for shard in range(devices)
        ]

    def offset(order, count):
        result = 0
        for i in range(count):
            result = result + bits[order[i]] * (devices >> (i + 1))
        return result

    def part(q, i, which):
        size, order = plan[q][2], plan[q][3]
        start = (offset(order, i) + which * (devices >> (i + 1))) * size
        return pl.ds(pl.multiple_of(start, 8), (devices >> (i + 1)) * size)

    def reduce_copy(q, i):
        k = plan[q][3][i]
        return remote(
            getattr(r, f"sum{q}").at[part(q, i, 1 - bits[k])], getattr(r, f"rget{q}_{i}"),
            r.rsem.at[0, i, q], r.rsem.at[1, i, q], partners[k],
        )

    def reduce_step(q, i):
        k = plan[q][3][i]
        reduce_copy(q, i).wait_recv()
        sums = getattr(r, f"sum{q}")
        mine = part(q, i, bits[k])
        sums[mine] = sums[mine] + getattr(r, f"rget{q}_{i}")[...]
        if i + 1 < levels:
            reduce_copy(q, i + 1).start()

    def send_piece(q):
        plane, first, size, order = plan[q]
        grad = r.gproj[:, plane * state_dim : (plane + 1) * state_dim]
        sums = getattr(r, f"sum{q}")
        where = places(order)
        product = mm(r.layer_t[devices * first : devices * (first + size)], grad)
        for shard in range(devices):
            sums[where[shard] * size : (where[shard] + 1) * size] = (
                product[shard * size : (shard + 1) * size])
        reduce_copy(q, 0).start()

    def finish_c():
        grad_c = r.gc[...] + mm_tn(r.gscores[...].astype(BF16), r.proj[:, :state_dim])
        grad_c = grad_c.astype(BF16)
        r.gproj[:, state_dim : 2 * state_dim] = grad_c

    def finish_b():
        grad_b = r.gb[...] + mm(r.gscores[...].astype(BF16), r.proj[:, state_dim:])
        grad_b = grad_b.astype(BF16)
        r.gproj[:, :state_dim] = grad_b

    def before_dt():
        upper = triangle(tokens, lambda a, b: a <= b)
        inner = r.rows[:, 0, :].T + r.reads[...] - r.cols[...]
        r.pre[...] = exact_mm(upper, inner)
        r.sigmoid[...] = 1.0 / (1.0 + jnp.exp(-r.raw[...]))

    def finish_dt():
        step = r.step[...]
        rate = jnp.exp(r.rate[...])
        total = r.run[tokens - 1 :, :]
        lower = triangle(tokens, lambda a, b: a > b)
        grad_decay = (
            r.pre[...] + exact_mm(lower, step * r.backs[...]) + jnp.exp(total) * r.cross[0:1]
        )
        grad_raw = (r.gsteps[...] - rate * grad_decay) * r.sigmoid[...]
        r.gproj[:, 2 * state_dim :] = grad_raw.astype(BF16)
        small = jnp.concatenate([
            jnp.sum(grad_raw, axis=0, keepdims=True),
            -rate * jnp.sum(grad_decay * step, axis=0, keepdims=True),
            r.skips[0:1],
            jnp.zeros((5, heads), F32),
        ], axis=0)
        r.small[...] = jnp.concatenate([small, jnp.zeros((8, TILE - heads), F32)], axis=1)

    def send_dt():
        narrow = r.gproj[:, 2 * state_dim :]
        product = mm(r.layer_t[...], jnp.concatenate(
            [narrow.astype(F32), jnp.zeros((tokens, TILE - heads), F32)], axis=1).astype(BF16))
        small = r.small[...]

        def shard_rows(shard, begin, count):
            found, first = [], 0
            for size in pieces_of(share):
                low, high = max(begin, first), min(begin + count, first + size)
                if low < high:
                    base = devices * first + shard * size - first
                    found.append(product[base + low : base + high])
                first += size
            return found[0] if len(found) == 1 else jnp.concatenate(found, axis=0)

        q = len(plan) - 1
        unit = group + 8
        sums = getattr(r, f"sum{q}")
        where = places(plan[q][3])
        for shard in range(devices):
            start = where[shard] * unit
            packed = jnp.zeros((group, TILE), F32)
            for j in range(lanes):
                count = min(share - j * group, group)
                if count <= 0:
                    continue
                piece = shard_rows(shard, j * group, count)
                if j > 0:
                    piece = pltpu.roll(piece, j * heads, 1)
                if count < group:
                    piece = jnp.concatenate(
                        [piece, jnp.zeros((group - count, TILE), F32)], axis=0)
                packed = packed + piece
            sums[start : start + group] = packed
            sums[start + group : start + unit] = small
        reduce_copy(q, 0).start()

    def layer_tail(k):
        cols = slice(k * depth // TAILS, (k + 1) * depth // TAILS)
        glayer_ref[:, cols] = (
            mm_nt(r.gproj[:, : 2 * state_dim], r.wbc[cols])
            + mm(r.gproj[:, 2 * state_dim :], r.wdt[:, cols])
        ).astype(BF16)

    def prepare():
        run = r.run[...]
        run_rows = run.T
        for head in range(heads):
            r.run_rows[head] = run_rows[head : head + 1]
        r.parts[...] = stacked(run)
        r.scores[...] = mm_nt(r.proj[:, :state_dim], r.proj[:, state_dim:])
        r.gscores[...] = jnp.zeros_like(r.gscores)

    def turn():
        turned = r.layer[...].T
        first = 0
        for size in pieces_of(share):
            for shard in range(devices):
                start, target = shard * share + first, devices * first + shard * size
                r.layer_t[target : target + size] = turned[start : start + size]
            first += size

    def body(pair, _):
        inner_pair(pair, heads, r.u, r.grad, r.scores, r.parts, r.run_rows,
                   r.gu, r.rows, r.gscores, head_size)
        return 0

    n = CHUNKS
    wire, flight, near, hop_wire, hop = 7.05 / n, 2.7, 1.0, 7.2 / (2 * n), 2.7 + 3.6 / n
    blocks = n // BLOCK
    pool, link = [], {"y": 0.0, "s": 0.0, "g": 0.0, "z": 0.0, "m": 0.0}
    clock, serial = [3.2], [0]
    left = {"s": n, "g": n}

    def add(ready, rank, cost, work, args=(), after=None):
        serial[0] += 1
        pool.append((ready, rank, serial[0], cost, work, args, after))

    def through(name, now, time):
        link[name] = max(link[name], now) + time
        return link[name]

    def after_make(kind, block):
        def after(now):
            for k in range(block * BLOCK, (block + 1) * BLOCK):
                add(now + near, 0, 0.02, pair_up, (kind, k), after_pair(kind, k))
        return after

    def after_pair(kind, k):
        def after(now):
            add(through("y", now, wire) + flight, 0, 0.02, row_up, (kind, k),
                lambda now: add(now, 0, 0.01, chain_slot, (kind, k, 0), after_chain(kind, k, 0)))
        return after

    def after_chain(kind, k, place):
        def after(now):
            if place + 1 < zrows:
                add(through(kind, now, hop_wire) + hop, 0, 0.01, chain_slot,
                    (kind, k, place + 1), after_chain(kind, k, place + 1))
            else:
                add(now, 0, 0.02, row_down, (kind, k), after_down(kind, k))
        return after

    def after_down(kind, k):
        def after(now):
            add(through("y", now, wire) + flight, 0, 0.02, chip_down, (kind, k),
                lambda now: add(now + near, 1, 4.1 / n if kind == "s" else 5.0 / n,
                                forward_tail if kind == "s" else backward_tail, (k,),
                                after_tail(kind)))
        return after

    def after_tail(kind):
        def after(now):
            left[kind] -= 1
            if left[kind] == 0:
                add(now, 1, 0.22, finish_c if kind == "s" else finish_b, (), after_finish(kind))
        return after

    def after_dt(now):
        add(now, 1, 0.9, send_dt, (), after_send(len(plan) - 1))
        for k in range(TAILS):
            soft.append((1.5 / TAILS, functools.partial(layer_tail, k)))

    def after_finish(kind):
        def after(now):
            for q, (plane, first, size, order) in enumerate(plan):
                if plane == (1 if kind == "s" else 0):
                    add(now, 1, size * 0.007, send_piece, (q,), after_send(q))
            if kind == "g":
                add(now + 0.01, 1, 0.31, finish_dt, (), after_dt)
        return after

    def after_send(q):
        arrive = near + (0.5 if plan[q][0] == 2 else 0.0)
        return lambda now: add(now + arrive, 0, 0.03, reduce_step, (q, 0), after_reduce(q, 0))

    def after_reduce(q, i):
        def after(now):
            if i + 1 == levels:
                return
            level = plan[q][3][i + 1]
            pace = plan[q][2] * 0.045 / (1 << i)
            if level == 1:
                arrive = through("y", now, pace) + 2.8
            elif level == 2:
                arrive = through("z", now, pace) + 2.8
            else:
                through("z", now, pace)
                arrive = through("m", now, 2 * pace) + 3.5
            if i + 2 == levels:
                arrive += 1000.0
            add(arrive, 0, 0.02, reduce_step, (q, i + 1), after_reduce(q, i + 1))
        return after

    for block in range(blocks):
        add(0.0, 1, 2.25 / blocks, make_states, ("s", block), after_make("s", block))
    for block in range(blocks):
        add(0.1, 1, 1.9 / blocks, make_states, ("g", block), after_make("g", block))
    add(4.0, 0, 0.25, tot_done, (0,))
    add(7.0, 0, 0.25, tot_done, (1,))

    pairs = width // TILE
    soft = [(0.25, prepare)] + [(0.46, None)] * pairs + [(0.4, turn)]
    soft += [(1.7 / n, functools.partial(inner_tail, k)) for k in range(n)] + [(0.4, before_dt)]
    pending = [0, 0]

    def flush_pairs():
        if pending[1]:
            lax.fori_loop(pending[0], pending[0] + pending[1], body, 0)
            pending[0], pending[1] = pending[0] + pending[1], 0

    def soften():
        cost, work = soft.pop(0)
        clock[0] += cost
        if work is None:
            pending[1] += 1
        else:
            flush_pairs()
            work()

    while pool:
        ready = [item for item in pool if item[0] <= clock[0] + 1e-6]
        if not ready:
            following = min(item[0] for item in pool)
            usable = soft and (soft[0][1] is not before_dt or left["s"] == 0)
            if usable and clock[0] + soft[0][0] <= following + 0.25:
                soften()
            else:
                clock[0] = following
            continue
        item = min(ready, key=lambda entry: (entry[1], entry[0], entry[2]))
        pool.remove(item)
        cost, work, args, after = item[3:]
        if work in (finish_c, backward_tail):
            while soft and soft[0][1] is not before_dt:
                soften()
        if work is finish_dt or item[0] > 1000.0:
            while soft:
                soften()
        flush_pairs()
        work(*args)
        clock[0] += cost
        if after:
            after(clock[0])

    for q, (plane, first, size, order) in enumerate(plan):
        unit = size
        start = pl.multiple_of(offset(order, levels) * unit, 8)
        result = getattr(r, f"sum{q}")[pl.ds(start, unit)]
        if plane < 2:
            gbc_ref[first : first + size, plane * TILE : (plane + 1) * TILE] = result
        else:
            last_ref[...] = result
    for k in range(2):
        tot_copy(k).wait_send()
    for kind in kinds:
        for k in range(n):
            for stage in (0, 1, 3, 4):
                copy(stage, kind, k).wait_send()
        if zrows > 1:
            sends = row < zrows - 1 if kind == "s" else row > 0

            @pl.when(sends)
            def _(kind=kind):
                for k in range(n):
                    copy(2, kind, k).wait_send()
    for q in range(len(plan)):
        for i in range(levels):
            reduce_copy(q, i).wait_send()


def finish_kernel(heads, group, lanes, gvalues_in, glayer_in, gbc_in, last_in,
                  gvalues_ref, glayer_ref, gbc_ref, gdt_ref, gbias_ref, grate_ref, gskip_ref, sems):
    copies = [
        pltpu.make_async_copy(source, target, sems.at[i])
        for i, (source, target) in enumerate((
            (gvalues_in, gvalues_ref), (glayer_in, glayer_ref), (gbc_in, gbc_ref),
        ))
    ]
    for copy in copies:
        copy.start()
    last = last_in[...]
    share = gdt_ref.shape[1]
    pieces = []
    for j in range(lanes):
        count = min(share - j * group, group)
        if count > 0:
            pieces.append(last[:count, j * heads : (j + 1) * heads])
    gdt_ref[...] = jnp.concatenate(pieces, axis=0).T
    gbias_ref[...] = last[group : group + 1, :heads]
    grate_ref[...] = last[group + 1 : group + 2, :heads]
    gskip_ref[...] = last[group + 2 : group + 3, :heads]
    for copy in copies:
        copy.wait()


def local(layer_in, ssm_in, weight_bc, weight_dt, bias_dt, log_rate, skip_gain, grad_out):
    tokens, depth = layer_in.shape
    heads = log_rate.shape[0]
    width = ssm_in.shape[1]
    state_dim = weight_bc.shape[1] // 2
    devices = lax.axis_size("seq")
    share, lanes, group = packing(depth, devices, heads)
    scratch = scratch_list(tokens, depth, width, heads, state_dim, devices)
    shape = jax.ShapeDtypeStruct
    gvalues, glayer, gbc, last = pl.pallas_call(
        functools.partial(mega_kernel, devices, list(scratch)),
        out_shape=[
            pltpu.VMEM((tokens, width), BF16),
            pltpu.VMEM((tokens, depth), BF16),
            pltpu.VMEM((share, 2 * state_dim), F32),
            pltpu.VMEM((group + 8, TILE), F32),
        ],
        in_specs=[ANY] * 8,
        out_specs=[VMEM, VMEM, VMEM, VMEM],
        scratch_shapes=list(scratch.values()),
        compiler_params=pltpu.CompilerParams(
            collective_id=0, has_side_effects=True, vmem_limit_bytes=VMEM_LIMIT
        ),
        name="mixer",
    )(layer_in, ssm_in, weight_bc, weight_dt.T, bias_dt[None, :], log_rate[None, :],
      skip_gain[None, :], grad_out)
    outs = pl.pallas_call(
        functools.partial(finish_kernel, heads, group, lanes),
        out_shape=[
            shape((tokens, width), BF16),
            shape((tokens, depth), BF16),
            shape((share, 2 * state_dim), F32),
            shape((heads, share), F32),
            shape((1, heads), F32),
            shape((1, heads), F32),
            shape((1, heads), F32),
        ],
        in_specs=[VMEM] * 4,
        out_specs=[ANY] * 3 + [VMEM] * 4,
        scratch_shapes=[pltpu.SemaphoreType.DMA((3,))],
        compiler_params=pltpu.CompilerParams(vmem_limit_bytes=8 * 1024 * 1024),
        name="finish",
    )(gvalues, glayer, gbc, last)
    return tuple(outs[:3]) + (outs[3].T,) + tuple(out[0] for out in outs[4:])


def solution(mesh):
    rows = P(("groups", "seq"), None)
    in_specs = (rows, rows, P(), P(), P(), P(), P(), rows)
    out_specs = (rows, rows, rows, rows, P("groups"), P("groups"), P("groups"))
    return jax.shard_map(local, mesh=mesh, in_specs=in_specs, out_specs=out_specs, check_vma=False)
```
